1024 devices in a mesh: agg: 8 (over y, core), gx: 32 (over z_lo, x), gy: 4 (over z_hi).
Axes of the slice: x: 4, y: 4, z: 32 (z_hi: 4, z_lo: 8; z = z_hi * 8 + z_lo), core: 2. Of those that a mesh axis runs over, the one named last changes fastest.
Arguments:
- velocity_prev: float32 [3, 256, 64, 1024], P(None, 'gx', 'gy', 'agg'), may hold values from -6 to 6
- forcing: float32 [3, 256, 64, 1024], P(None, 'gx', 'gy', 'agg'), may hold values from -6 to 6
- reaction: float32 [256, 64, 1024], P('gx', 'gy', 'agg'), may hold values from 0.1 to 4
Outputs:
- velocity: float32 [3, 256, 64, 1024], P(None, 'gx', 'gy', 'agg')
- compressed: float32 [3, 64, 1024, 128], P(None, 'gy', ('agg', 'gx'))
The draws below stay inside these ranges and needn't reach their ends.
All inputs are finite; a program needn't handle non-finite values.
Results may differ from the reference program's by a relative error of at most 0.00002.
Values sent between devices are 32-bit elements; how exact they have to be, the bound alone decides.
A program may use at most 64 MiB of HBM per device.

```python
import math
import jax
import jax.numpy as jnp
from jax import lax

SWEEPS = 2
COARSE_SWEEPS = 4
LX = 5
NX = 256
NY = 64
NZ = 1024


def shard_levels(rng, dims, cuts, low, top_value):
    loudness, own = 1.0, jax.random.fold_in(rng, 6)
    for axis_at, blocks in cuts:
        heights = jnp.exp(jax.random.uniform(jax.random.fold_in(own, axis_at), (blocks,), jnp.float32, low / len(cuts), top_value / len(cuts)))
        loudness = loudness * jnp.repeat(heights, dims[axis_at] // blocks).reshape([-1 if axis == axis_at else 1 for axis in range(len(dims))])
    return loudness


def normal_values(key, shape, scale, limit, split=(), kind=jnp.bfloat16):
    result = jax.random.normal(key, shape, jnp.float32) * scale
    if len(split) > 0:
        result = shard_levels(key, shape, split, -0.22, 0.18) * result
    return jnp.clip(result, min=-limit, max=limit).astype(kind)


def setup_inputs(seed: int = 0) -> dict:
    key_list = jax.random.split(jax.random.key(seed), 4)
    velocity_prev = normal_values(key_list[0], (3, NX, NY, NZ), 1.0, 6.0, ((1, 32), (2, 4), (3, 8)), jnp.float32)
    forcing = normal_values(key_list[1], (3, NX, NY, NZ), 1.0, 6.0, ((1, 32), (2, 4), (3, 8)), jnp.float32)
    reaction = jnp.clip(jnp.exp(math.log(4.0) - 3.6888794 * jax.random.uniform(key_list[2], (NX, NY, NZ), jnp.float32) ** shard_levels(key_list[2], (NX, NY, NZ), ((0, 32), (1, 4), (2, 8)), -0.2, 0.2)), 0.1, 4.0)
    return dict(velocity_prev=velocity_prev, forcing=forcing, reaction=reaction)


damping = 0.8
root_half = 0.7071067811865476


def neighbours(field):
    padded = jnp.pad(field, 1)
    summed = padded[2:, 1:-1, 1:-1] + padded[:-2, 1:-1, 1:-1]
    summed = summed + padded[1:-1, 2:, 1:-1] + padded[1:-1, :-2, 1:-1]
    summed = summed + padded[1:-1, 1:-1, 2:] + padded[1:-1, 1:-1, :-2]
    return summed


def fine_residual(current, forcing_part, diagonal):
    return forcing_part - (diagonal * current - neighbours(current))


def block_mean(field):
    size_x, size_y, size_z = field.shape
    return field.reshape(size_x // 2, 2, size_y // 2, 2, size_z // 2, 2).mean(axis=(1, 3, 5))


def prolong(coarse):
    size_x, size_y, size_z = coarse.shape
    expanded = jnp.broadcast_to(coarse[:, None, :, None, :, None], (size_x, 2, size_y, 2, size_z, 2))
    return expanded.reshape(2 * size_x, 2 * size_y, 2 * size_z)


def halve_last(values):
    paired = values.reshape(values.shape[:-1] + (values.shape[-1] // 2, 2))
    even_cells = paired[..., 0]
    odd_cells = paired[..., 1]
    return (even_cells + odd_cells) * root_half, (even_cells - odd_cells) * root_half


def x_levels(approx):
    details = []
    for level_index in range(LX - 1):
        approx, detail = halve_last(approx)
        details.append(detail)
    return jnp.concatenate([approx] + details[::-1], axis=-1)


def pair_pass(values, which_dim):
    layout = values.shape
    paired = values.reshape(layout[:which_dim] + (layout[which_dim] // 2, 2) + layout[which_dim + 1:])
    even_cells = lax.index_in_dim(paired, 0, which_dim + 1, keepdims=False)
    odd_cells = lax.index_in_dim(paired, 1, which_dim + 1, keepdims=False)
    stacked = jnp.stack([(even_cells + odd_cells) * root_half, (even_cells - odd_cells) * root_half], axis=which_dim + 1)
    return stacked.reshape(layout)


def reference(velocity_prev, forcing, reaction):
    diagonal = 6.0 + reaction
    coarse_diag = (6.0 + 4.0 * block_mean(reaction)) * 0.25

    def solve_component(inputs):
        previous, forcing_part = inputs
        current = previous
        for sweep_index in range(SWEEPS):
            current = current + damping * fine_residual(current, forcing_part, diagonal) / diagonal
        coarse_rhs = block_mean(fine_residual(current, forcing_part, diagonal))
        correction = damping * coarse_rhs / coarse_diag
        for sweep_index in range(COARSE_SWEEPS - 1):
            correction = correction + damping * (coarse_rhs - (coarse_diag * correction - 0.25 * neighbours(correction))) / coarse_diag
        current = current + prolong(correction)
        current = current + damping * fine_residual(current, forcing_part, diagonal) / diagonal
        x_lines = jnp.transpose(previous, (1, 2, 0))
        coeffs = x_levels(halve_last(x_lines)[0])
        coeffs = pair_pass(pair_pass(coeffs, 0), 1)
        return current, coeffs

    velocity, compressed = lax.map(solve_component, (velocity_prev, forcing))
    return velocity, compressed
```

```python
import functools

import jax
import jax.numpy as jnp
import numpy as np
from jax import lax
from jax.experimental import pallas as pl
from jax.experimental.pallas import tpu as pltpu
from jax.sharding import PartitionSpec as P

SWEEPS = 2
COARSE_SWEEPS = 4
LX = 5
damping = 0.8
keep = 1.0 - damping
root_half = 0.7071067811865476
MESH = pl.DeviceIdType.MESH
F32 = jnp.float32

X1, Z1, Y1, Y2, X2, XE, Z2, X3, Z3, DZ, DX, DY, BZ, BX, BY, COUNT = range(16)


def haar_matrix(devices):
    size = 4 * devices
    approx = np.eye(size)
    details = []
    for _ in range(LX - 1):
        even, odd = approx[:, 0::2], approx[:, 1::2]
        approx, detail = (even + odd) * root_half, (even - odd) * root_half
        details.append(detail)
    whole = np.concatenate([approx] + details[::-1], axis=1)
    parts = whole.reshape(devices, 4, size)
    return np.concatenate([parts[:, m] for m in range(4)], axis=1).astype(np.float32)


def dot(a, b, dims=((1,), (0,))):
    return lax.dot_general(
        a, b, (dims, ((), ())), precision=lax.Precision.HIGHEST, preferred_element_type=F32
    )


def lanes(shape):
    return lax.broadcasted_iota(jnp.int32, shape, len(shape) - 1)


def rows(shape):
    return lax.broadcasted_iota(jnp.int32, shape, len(shape) - 2)


def kernel(
    sizes, vp, f, r, mcat, vel, comp,
    c_ref, u1, u2, gb, tp, uh1, uh2, sendt, recvt,
    xs, xr1, xr2, xr3, xes, xer, zs1, zr1, zs2, zr2, zs3, zr3,
    y1s, y1r, y2s, y2r,
    down, dzr, dext, dxr, dys, dyr, dds, ddr,
    bown, bzr, bext, bxr, bys, byr, bds, bdr,
    ddiag, cdext, cf, cz, eu, ph,
    ssem, rsem, dssem, drsem, assem, arsem,
):
    n_agg, n_gx, n_gy = sizes
    per = 128 // n_gx
    axes = {"agg": n_agg, "gx": n_gx, "gy": n_gy}
    here = {name: lax.axis_index(name) for name in axes}

    def wrap(name, step):
        return lax.rem(here[name] + step + axes[name], axes[name])

    for ref in (xr1, xr2, xr3, xer, zr1, zr2, zr3, y1r, y2r, dzr, dxr, dyr, ddr, bzr, bxr, byr, bdr):
        ref[...] = jnp.zeros(ref.shape, F32)

    barrier = pltpu.get_barrier_semaphore()

    def greet(step, carry):
        pl.semaphore_signal(
            barrier, inc=1, device_id={"gx": lax.rem(here["gx"] + step, n_gx)}, device_id_type=MESH
        )
        return carry

    lax.fori_loop(1, n_gx, greet, 0)
    for name in ("gy", "agg"):
        for step in (1, -1):
            pl.semaphore_signal(barrier, inc=1, device_id={name: wrap(name, step)}, device_id_type=MESH)
    for sx in (1, -1):
        for sy in (1, -1):
            pl.semaphore_signal(
                barrier, inc=1, device_id={"gx": wrap("gx", sx), "gy": wrap("gy", sy)}, device_id_type=MESH
            )

    def pair_copy(message, axis, src, dst, side):
        step = 1 if side == 0 else -1
        return pltpu.make_async_remote_copy(
            src_ref=src.at[side], dst_ref=dst.at[side],
            send_sem=ssem.at[message, side], recv_sem=rsem.at[message, side],
            device_id={axis: here[axis] + step}, device_id_type=MESH,
        )

    def whole_copy(message, axis, src, dst, side):
        step = 1 if side == 0 else -1
        return pltpu.make_async_remote_copy(
            src_ref=src, dst_ref=dst.at[side],
            send_sem=ssem.at[message, side], recv_sem=rsem.at[message, side],
            device_id={axis: here[axis] + step}, device_id_type=MESH,
        )

    ends = []

    def start(message, axis, src, dst, make=pair_copy):
        @pl.when(here[axis] < axes[axis] - 1)
        def _():
            make(message, axis, src, dst, 0).start()

        @pl.when(here[axis] > 0)
        def _():
            make(message, axis, src, dst, 1).start()

        ends.append((message, axis, src, dst, make))

    def arrive(message, axis, src, dst, make=pair_copy):
        @pl.when(here[axis] > 0)
        def _():
            make(message, axis, src, dst, 0).wait_recv()

        @pl.when(here[axis] < axes[axis] - 1)
        def _():
            make(message, axis, src, dst, 1).wait_recv()

    def corner_copy(kind, src, dst, xs_, ys_):
        sx, sy = 1 if xs_ == 0 else -1, 1 if ys_ == 0 else -1
        k = xs_ * 2 + ys_
        return pltpu.make_async_remote_copy(
            src_ref=src.at[k], dst_ref=dst.at[k],
            send_sem=dssem.at[kind, k], recv_sem=drsem.at[kind, k],
            device_id={"gx": here["gx"] + sx, "gy": here["gy"] + sy}, device_id_type=MESH,
        )

    def has(axis, side):
        return here[axis] < axes[axis] - 1 if side == 0 else here[axis] > 0

    def from_(axis, side):
        return here[axis] > 0 if side == 0 else here[axis] < axes[axis] - 1

    def corners(kind, src, dst, verb):
        for xs_ in (0, 1):
            for ys_ in (0, 1):
                test = from_ if verb == "recv" else has

                @pl.when(jnp.logical_and(test("gx", xs_), test("gy", ys_)))
                def _(xs_=xs_, ys_=ys_):
                    copy = corner_copy(kind, src, dst, xs_, ys_)
                    if verb == "start":
                        copy.start()
                    elif verb == "recv":
                        copy.wait_recv()
                    else:
                        copy.wait_send()

    lane8, lane16, lane128 = lanes((8, 128)), lanes((16, 128)), lanes((128, 128))
    sub8 = rows((8, 128))
    y_at = lax.rem(rows((128, 128)), 16)

    def comp_of(ref, c):
        return ref[c * 128 : (c + 1) * 128, :]

    def plane(ref, c, j):
        return ref[pl.ds(c * 128 + j, 8, stride=16), :]

    def put_plane(ref, c, j, value):
        ref[pl.ds(c * 128 + j, 8, stride=16), :] = value

    def z_pack(tiles, column, lane):
        packed = jnp.zeros(lane.shape, F32)
        for place, tile in enumerate(tiles):
            packed = jnp.where(lane == place, pltpu.roll(tile, (place - column) % 128, 1), packed)
        return packed

    def z_tiles(ref):
        return [ref[t * 16 : (t + 1) * 16, :] for t in range(24)]

    def x_stage(ref):
        for c in range(3):
            xs_value = ref[c * 128 + 112 : c * 128 + 128, :]
            xs[stage, 0, c] = xs_value
            xs[stage, 1, c] = ref[c * 128 : c * 128 + 16, :]

    def spread(packed, c, lane_at):
        return jnp.concatenate(
            [pltpu.roll(packed, (lane_at - (c * 8 + x)) % 128, 1) for x in range(8)], axis=0
        )

    def around(u, x_low, x_high, z_low, z_high):
        total = jnp.concatenate([x_low, u[:112]], axis=0) + jnp.concatenate([u[16:], x_high], axis=0)
        total = total + jnp.where(lane128 == 0, z_low, pltpu.roll(u, 1, 1))
        total = total + jnp.where(lane128 == 127, z_high, pltpu.roll(u, 127, 1))
        total = total + jnp.where(y_at == 0, 0.0, pltpu.roll(u, 1, 0))
        return total + jnp.where(y_at == 15, 0.0, pltpu.roll(u, 127, 0))

    reaction = r[...]
    c_ref[...] = damping / (6.0 + reaction)
    for c in range(3):
        for side, j in ((0, 15), (1, 0)):
            y1s[side, c] = plane(vp, c, j)
    for side, j in ((0, 15), (1, 0)):
        y1s[side, 3] = c_ref[pl.ds(j, 8, stride=16), :]
    stage = 0
    x_stage(vp)
    zs1[0] = z_pack(z_tiles(vp), 127, lane16)
    zs1[1] = z_pack(z_tiles(vp), 0, lane16)

    halves = jnp.where(lax.shift_right_logical(rows((128, 128)), 1) == lane128, 0.125, 0.0)
    pairs = reaction.reshape(4, 2, 16, 128)
    tp[0:64, :] = (pairs[:, 0] + pairs[:, 1]).reshape(64, 128)
    mean_r = dot(tp[pl.ds(0, 32, stride=2), :] + tp[pl.ds(1, 32, stride=2), :], halves)
    inverse = damping / ((6.0 + 4.0 * mean_r) * 0.25)
    down[...] = jnp.where(lanes((32, 128)) < 64, inverse, 0.0).reshape(4, 8, 128)

    row192 = rows((192, 128))
    first = []
    for c in range(3):
        both = comp_of(vp, c).reshape(4, 2, 16, 128)
        first.append(((both[:, 0] + both[:, 1]) * root_half).reshape(64, 128))
    a1 = jnp.concatenate(first, axis=0)
    even = lax.rem(row192, 2) == 0
    a1 = jnp.where(even, a1 + pltpu.roll(a1, 191, 0), pltpu.roll(a1, 1, 0) - a1) * root_half
    out_z, in_z = rows((128, 128)), lane128
    same = lax.shift_right_logical(out_z, 1) == lax.shift_right_logical(in_z, 1)
    minus = jnp.logical_and(lax.rem(out_z, 2) == 1, lax.rem(in_z, 2) == 1)
    pass_z = jnp.where(same, jnp.where(minus, -root_half, root_half), 0.0).astype(F32)
    turned = jnp.concatenate([dot(pass_z, a1, ((1,), (1,))), jnp.zeros((128, 64), F32)], axis=1)
    for t in range(n_gx):
        sendt[t] = turned[t * per : (t + 1) * per, :]

    pl.semaphore_wait(barrier, n_gx - 1 + 8)

    start(Y1, "gy", y1s, y1r)
    start(X1, "gx", xs.at[0], xr1)
    start(Z1, "agg", zs1, zr1)
    start(DZ, "agg", down, dzr, whole_copy)
    arrive(X1, "gx", xs.at[0], xr1)
    arrive(Z1, "agg", zs1, zr1)
    z_low, z_high = zr1[0], zr1[1]
    for c in range(3):
        u = comp_of(vp, c)
        total = comp_of(f, c) + around(
            u, xr1[0, c], xr1[1, c], spread(z_low, c, 0), spread(z_high, c, 127)
        )
        gb[c * 128 : (c + 1) * 128, :] = total
        u1[c * 128 : (c + 1) * 128, :] = keep * u + c_ref[...] * total
    for c in range(3):
        for side, j, inner in ((0, 15, 14), (1, 0, 1)):
            y2s[side, c] = plane(gb, c, j)
            y2s[side, 3 + c] = plane(f, c, j) + plane(u1, c, inner)
    start(Y2, "gy", y2s, y2r)

    def widen(own, received, wide, n):
        lane = lanes((n * 8, 128))
        mine = own[...].reshape(n * 8, 128)
        low, high = received[0].reshape(n * 8, 128), received[1].reshape(n * 8, 128)
        turned_ = pltpu.roll(jnp.where(lane < 32, high, low), 64, 1)
        edge = jnp.logical_or(lane < 68, lane >= 124)
        value = jnp.where(lane < 64, mine, jnp.where(edge, turned_, 0.0))
        wide[...] = value.reshape(n, 8, 128)

    def stage_rows(wide, y_stage, corner_stage, n):
        for c in range(n):
            for half in range(2):
                a, b = wide[c * 4 + 2 * half], wide[c * 4 + 2 * half + 1]
                y_stage[0, c * 2 + half] = jnp.where(sub8 < 4, pltpu.roll(a, 4, 0), b)
                y_stage[1, c * 2 + half] = jnp.where(sub8 < 4, a, pltpu.roll(b, 4, 0))
            for xs_ in (0, 1):
                order = (3, 2, 1) if xs_ == 0 else (0, 1, 2)
                one, two, three = (wide[c * 4 + i] for i in order)
                corner_stage[xs_ * 2, c] = jnp.where(
                    sub8 >= 4, one, jnp.where(sub8 >= 2, pltpu.roll(two, 4, 0), pltpu.roll(three, 1, 0))
                )
                corner_stage[xs_ * 2 + 1, c] = jnp.where(
                    sub8 < 4, one, jnp.where(sub8 < 6, pltpu.roll(two, 4, 0), pltpu.roll(three, 7, 0))
                )

    def assemble(wide, x_got, y_got, corner_got, c):
        tiles = []
        for place in range(12):
            if 4 <= place < 8:
                i = place - 4
                main = wide[c * 4 + i]
                high, low = y_got[1, c * 2 + i // 2], y_got[0, c * 2 + i // 2]
                if i % 2 == 0:
                    halo = jnp.where(sub8 < 4, high, pltpu.roll(low, 4, 0))
                else:
                    halo = jnp.where(sub8 < 4, pltpu.roll(high, 4, 0), low)
            else:
                side = 0 if place < 4 else 1
                away = 4 - place if side == 0 else place - 7
                main = x_got[side, c * 4 + (place if side == 0 else place - 8)]
                if away == 4:
                    halo = jnp.zeros((8, 128), F32)
                else:
                    low, high = corner_got[side * 2, c], corner_got[side * 2 + 1, c]
                    if away == 1:
                        halo = jnp.where(sub8 < 4, high, low)
                    elif away == 2:
                        halo = jnp.where(
                            sub8 < 2, pltpu.roll(high, 4, 0),
                            jnp.where(sub8 >= 6, pltpu.roll(low, 4, 0), 0.0),
                        )
                    else:
                        halo = jnp.where(
                            sub8 == 0, pltpu.roll(high, 1, 0),
                            jnp.where(sub8 == 7, pltpu.roll(low, 7, 0), 0.0),
                        )
            tiles += [main, halo]
        return jnp.concatenate(tiles, axis=0)

    arrive(DZ, "agg", down, dzr, whole_copy)
    widen(down, dzr, dext, 4)
    stage_rows(dext, dys, dds, 1)
    start(DX, "gx", dext, dxr, whole_copy)
    start(DY, "gy", dys, dyr)
    corners(0, dds, ddr, "start")

    arrive(Y1, "gy", y1s, y1r)
    for c in range(3):
        for side, j in ((0, 0), (1, 15)):
            put_plane(u1, c, j, plane(u1, c, j) + c_ref[pl.ds(j, 8, stride=16), :] * y1r[side, c])
    arrive(Y2, "gy", y2s, y2r)
    for c in range(3):
        for side, j in ((0, 0), (1, 15)):
            at = (side * 3 + c) * 8
            uh1[at : at + 8, :] = keep * y1r[side, c] + y1r[side, 3] * (y2r[side, c] + plane(vp, c, j))

    stage = 1
    x_stage(u1)
    xes[0, 0:6, :] = uh1[pl.ds(7, 6, stride=8), :]
    xes[1, 0:6, :] = uh1[pl.ds(0, 6, stride=8), :]
    start(X2, "gx", xs.at[1], xr2)
    start(XE, "gx", xes, xer)
    edge_tiles = [uh1[t * 8 : (t + 1) * 8, :] for t in range(6)]
    zs2[0, 0:16, :] = z_pack(z_tiles(u1), 127, lane16)
    zs2[0, 16:24, :] = z_pack(edge_tiles, 127, lane8)
    zs2[1, 0:16, :] = z_pack(z_tiles(u1), 0, lane16)
    zs2[1, 16:24, :] = z_pack(edge_tiles, 0, lane8)
    start(Z2, "agg", zs2, zr2)

    def line_copy(step):
        target = lax.rem(here["gx"] + step, n_gx)
        return pltpu.make_async_remote_copy(
            src_ref=sendt.at[target], dst_ref=recvt.at[here["gx"]],
            send_sem=assem, recv_sem=arsem, device_id={"gx": target}, device_id_type=MESH,
        )

    def send_line(step, carry):
        line_copy(step).start()
        return carry

    lax.fori_loop(1, n_gx, send_line, 0)

    arrive(X2, "gx", xs.at[1], xr2)
    arrive(XE, "gx", xes, xer)
    arrive(Z2, "agg", zs2, zr2)
    z_low, z_high = zr2[0, 0:16, :], zr2[1, 0:16, :]
    for c in range(3):
        u = comp_of(u1, c)
        total = comp_of(f, c) + around(
            u, xr2[0, c], xr2[1, c], spread(z_low, c, 0), spread(z_high, c, 127)
        )
        u2[c * 128 : (c + 1) * 128, :] = keep * u + c_ref[...] * total
    edge_low, edge_high = zr2[0, 16:24, :], zr2[1, 16:24, :]
    for c in range(3):
        for side, j in ((0, 0), (1, 15)):
            k = side * 3 + c
            at = k * 8
            p = uh1[at : at + 8, :]
            put_plane(u2, c, j, plane(u2, c, j) + c_ref[pl.ds(j, 8, stride=16), :] * p)
            near = jnp.where(sub8 == 0, xer[0, k : k + 1, :], pltpu.roll(p, 1, 0))
            near = near + jnp.where(sub8 == 7, xer[1, k : k + 1, :], pltpu.roll(p, 7, 0))
            near = near + jnp.where(lane8 == 0, pltpu.roll(edge_low, (-k) % 128, 1), pltpu.roll(p, 1, 1))
            near = near + jnp.where(
                lane8 == 127, pltpu.roll(edge_high, 127 - k, 1), pltpu.roll(p, 127, 1)
            )
            uh2[at : at + 8, :] = keep * p + y1r[side, 3] * (y2r[side, 3 + c] + near + plane(u1, c, j))

    stage = 2
    x_stage(u2)
    start(X3, "gx", xs.at[2], xr3)
    zs3[0] = z_pack(z_tiles(u2), 127, lane16)
    zs3[1] = z_pack(z_tiles(u2), 0, lane16)
    start(Z3, "agg", zs3, zr3)

    arrive(DX, "gx", dext, dxr, whole_copy)
    arrive(DY, "gy", dys, dyr)
    corners(0, dds, ddr, "recv")
    cdext[...] = assemble(dext, dxr, dyr, ddr, 0)

    arrive(X3, "gx", xs.at[2], xr3)
    arrive(Z3, "agg", zs3, zr3)
    z_low, z_high = zr3[0], zr3[1]
    for c in range(3):
        u = comp_of(u2, c)
        gb[c * 128 : (c + 1) * 128, :] = (
            comp_of(f, c) - (6.0 + r[...]) * u
            + around(u, xr3[0, c], xr3[1, c], spread(z_low, c, 0), spread(z_high, c, 127))
        )
    for c in range(3):
        for side, j in ((0, 0), (1, 15)):
            at = (side * 3 + c) * 8
            put_plane(gb, c, j, plane(gb, c, j) + uh2[at : at + 8, :])
    for c in range(3):
        both = comp_of(gb, c).reshape(4, 2, 16, 128)
        tp[c * 64 : (c + 1) * 64, :] = (both[:, 0] + both[:, 1]).reshape(64, 128)
    rhs = dot(tp[pl.ds(0, 96, stride=2), :] + tp[pl.ds(1, 96, stride=2), :], halves)
    bown[...] = rhs.reshape(12, 8, 128)
    start(BZ, "agg", bown, bzr, whole_copy)
    arrive(BZ, "agg", bown, bzr, whole_copy)
    widen(bown, bzr, bext, 12)
    stage_rows(bext, bys, bds, 3)
    start(BY, "gy", bys, byr)
    corners(1, bds, bdr, "start")
    start(BX, "gx", bext, bxr, whole_copy)

    many = n_gx - 1
    lines = pltpu.make_async_remote_copy(
        src_ref=sendt.at[pl.ds(0, many)], dst_ref=recvt.at[pl.ds(0, many)],
        send_sem=assem, recv_sem=arsem, device_id={"gx": wrap("gx", 1)}, device_id_type=MESH,
    )
    lines.wait_recv()
    lines.wait_send()
    recvt[here["gx"]] = sendt[here["gx"]]
    for k in range(per):
        got = recvt[:, k, :]
        wide = dot(got[:, 0:192], mcat[...], ((0,), (0,)))
        for c in range(3):
            value = 0.0
            for m in range(4):
                at = (c * 4 + m) * 16
                value = value + wide[at : at + 16, m * 4 * n_gx : (m + 1) * 4 * n_gx]
            comp[k, c] = value

    arrive(BX, "gx", bext, bxr, whole_copy)
    arrive(BY, "gy", bys, byr)
    corners(1, bds, bdr, "recv")

    y16 = lax.rem(rows((192, 128)), 16)
    fine = lane128 // 2 == rows((128, 128))
    beyond = jnp.logical_or(
        jnp.logical_and(lane128 == 0, rows((128, 128)) == 127),
        jnp.logical_and(lane128 == 127, rows((128, 128)) == 64),
    )
    up = jnp.concatenate([jnp.where(fine, 1.0, 0.0), jnp.where(beyond, 1.0, 0.0)], axis=1).astype(F32)
    none = jnp.zeros((16, 128), F32)
    for c in range(3):
        rhs_c = assemble(bext, bxr, byr, bdr, c)
        weight = cdext[...]
        e = weight * rhs_c
        for _ in range(COARSE_SWEEPS - 1):
            near = jnp.concatenate([none, e[:176]], axis=0) + jnp.concatenate([e[16:], none], axis=0)
            near = near + pltpu.roll(e, 1, 1) + pltpu.roll(e, 127, 1)
            near = near + jnp.where(y16 == 0, pltpu.roll(e, 192 - 15, 0), pltpu.roll(e, 1, 0))
            near = near + jnp.where(y16 == 15, pltpu.roll(e, 15, 0), pltpu.roll(e, 191, 0))
            e = keep * e + weight * (rhs_c + 0.25 * near)
        refined = dot(e[48:144], up)
        eu[c * 96 : (c + 1) * 96, :] = refined[:, 0:128]
        for ref, part in ((cf, refined[:, 0:128]), (cz, refined[:, 128:256])):
            main = part.reshape(6, 16, 128)[:, 0:8].reshape(48, 128)
            ref[pl.ds(c * 96, 48, stride=2), :] = main
            ref[pl.ds(c * 96 + 1, 48, stride=2), :] = main
        for side, row in ((0, 15), (1, 8)):
            line = eu[pl.ds(c * 96 + 16 + row, 4, stride=16), :]
            at = (side * 3 + c) * 8
            ph[pl.ds(at, 4, stride=2), :] = line
            ph[pl.ds(at + 1, 4, stride=2), :] = line

    def doubled(ref, c):
        value = ref[c * 96 + 16 : c * 96 + 80, :].reshape(4, 1, 16, 128)
        return jnp.broadcast_to(value, (4, 2, 16, 128)).reshape(128, 128)

    for c in range(3):
        w = comp_of(u2, c) + doubled(cf, c)
        beside = doubled(cz, c)
        total = comp_of(f, c) + around(
            w,
            xr3[0, c] + cf[c * 96 : c * 96 + 16, :],
            xr3[1, c] + cf[c * 96 + 80 : c * 96 + 96, :],
            spread(z_low, c, 0) + beside,
            spread(z_high, c, 127) + beside,
        )
        vel[c * 128 : (c + 1) * 128, :] = keep * w + c_ref[...] * total
    for c in range(3):
        for side, j in ((0, 0), (1, 15)):
            at = (side * 3 + c) * 8
            beyond_y = uh2[at : at + 8, :] + ph[at : at + 8, :]
            put_plane(vel, c, j, plane(vel, c, j) + c_ref[pl.ds(j, 8, stride=16), :] * beyond_y)

    for message, axis, src, dst, make in ends:

        @pl.when(here[axis] < axes[axis] - 1)
        def _(args=(message, axis, src, dst), make=make):
            make(*args, 0).wait_send()

        @pl.when(here[axis] > 0)
        def _(args=(message, axis, src, dst), make=make):
            make(*args, 1).wait_send()

    corners(0, dds, ddr, "send")
    corners(1, bds, bdr, "send")


def on_device(sizes, velocity_prev, forcing, reaction):
    n_agg, n_gx, n_gy = sizes
    per = 128 // n_gx
    v = pltpu.VMEM
    scratch = [
        v((128, 128), F32), v((384, 128), F32), v((384, 128), F32), v((384, 128), F32),
        v((192, 128), F32), v((48, 128), F32), v((48, 128), F32),
        v((n_gx, per, 256), F32), v((n_gx, per, 256), F32),
        v((3, 2, 3, 16, 128), F32), v((2, 3, 16, 128), F32), v((2, 3, 16, 128), F32), v((2, 3, 16, 128), F32),
        v((2, 8, 128), F32), v((2, 8, 128), F32),
        v((2, 16, 128), F32), v((2, 16, 128), F32), v((2, 24, 128), F32), v((2, 24, 128), F32),
        v((2, 16, 128), F32), v((2, 16, 128), F32),
        v((2, 4, 8, 128), F32), v((2, 4, 8, 128), F32), v((2, 6, 8, 128), F32), v((2, 6, 8, 128), F32),
    ]
    for n in (1, 3):
        scratch += [
            v((n * 4, 8, 128), F32), v((2, n * 4, 8, 128), F32), v((n * 4, 8, 128), F32),
            v((2, n * 4, 8, 128), F32), v((2, n * 2, 8, 128), F32), v((2, n * 2, 8, 128), F32),
            v((4, n, 8, 128), F32), v((4, n, 8, 128), F32),
        ]
    scratch += [
        v((8, 128), F32), v((192, 128), F32), v((288, 128), F32), v((288, 128), F32), v((288, 128), F32),
        v((48, 128), F32),
        pltpu.SemaphoreType.DMA((COUNT, 2)), pltpu.SemaphoreType.DMA((COUNT, 2)),
        pltpu.SemaphoreType.DMA((2, 4)), pltpu.SemaphoreType.DMA((2, 4)),
        pltpu.SemaphoreType.DMA, pltpu.SemaphoreType.DMA,
    ]
    vmem = pl.BlockSpec(memory_space=pltpu.VMEM)
    velocity, compressed = pl.pallas_call(
        functools.partial(kernel, sizes),
        out_shape=(
            jax.ShapeDtypeStruct((384, 128), F32),
            jax.ShapeDtypeStruct((per, 3, 16, 4 * n_gx), F32),
        ),
        in_specs=[vmem] * 4,
        out_specs=(vmem, vmem),
        scratch_shapes=scratch,
        compiler_params=pltpu.CompilerParams(collective_id=0, has_side_effects=True),
        name="vcycle",
    )(
        velocity_prev.reshape(384, 128), forcing.reshape(384, 128), reaction.reshape(128, 128),
        jnp.asarray(haar_matrix(n_gx)),
    )
    return velocity.reshape(3, 8, 16, 128), jnp.transpose(compressed, (1, 2, 0, 3))


def solution(mesh):
    placed = (P(None, "gx", "gy", "agg"), P(None, "gx", "gy", "agg"), P("gx", "gy", "agg"))
    sizes = tuple(mesh.shape[name] for name in ("agg", "gx", "gy"))
    return jax.shard_map(
        functools.partial(on_device, sizes),
        mesh=mesh,
        in_specs=placed,
        out_specs=(P(None, "gx", "gy", "agg"), P(None, "gy", ("agg", "gx"), None)),
        check_vma=False,
    )
```

```python
import functools

import jax
import jax.numpy as jnp
import numpy as np
from jax import lax
from jax.experimental import pallas as pl
from jax.experimental.pallas import tpu as pltpu
from jax.sharding import PartitionSpec as P

SWEEPS = 2
COARSE_SWEEPS = 4
LX = 5
damping = 0.8
keep = 1.0 - damping
root_half = 0.7071067811865476
MESH = pl.DeviceIdType.MESH
F32 = jnp.float32

X1, Z1, X2, Z2, X3, Z3, XF2, ZF2, XF3, ZF3, DZ, DX, DXZ, BZ, BX, BXZ, Y1, Y2, Y3, Y4, COUNT = range(21)
ROW = 4
TURNS = (1, 1, 2, 2, 3, 3, 4, 5)

def haar_matrix(devices):
    size = 4 * devices
    approx = np.eye(size)
    details = []
    for _ in range(LX - 1):
        even, odd = approx[:, 0::2], approx[:, 1::2]
        approx, detail = (even + odd) * root_half, (even - odd) * root_half
        details.append(detail)
    whole = np.concatenate([approx] + details[::-1], axis=1)
    parts = whole.reshape(devices, 4, size)
    return np.concatenate([parts[:, m] for m in range(4)], axis=1).astype(np.float32)


def dot(a, b, dims=((1,), (0,))):
    return lax.dot_general(
        a, b, (dims, ((), ())), precision=lax.Precision.HIGHEST, preferred_element_type=F32
    )


def lanes(shape):
    return lax.broadcasted_iota(jnp.int32, shape, len(shape) - 1)


def rows(shape):
    return lax.broadcasted_iota(jnp.int32, shape, len(shape) - 2)


def kernel(
    sizes, vp_in, f_in, r_in, m_in, vel, comp,
    vp, f, r, mcat, c_ref, u1, u2, uz, gb, tp, sendt, recvt,
    xs, xr1, xr2, xr3, zs1, zr1, zs2, zr2, zs3, zr3,
    p1, p2, ps, xf2s, xf2r, zf2s, zf2r, xf3s, xf3r, zf3s, zf3r,
    y1s, y1r, y2s, y2r, y3s, y3r, y4s, y4r,
    down, dtile, dpack, dxr, dzs, dzr, dxz, bown, btile, bpack, bxr, bzs, bzr, bxz,
    cdext, cf, cz, eu, ph,
    insem, ssem, rsem, assem, arsem, ready, token_up, token_down,
):
    n_agg, n_gx, n_gy = sizes
    per = 128 // n_gx
    levels = n_gx // ROW
    axes = {"agg": n_agg, "gx": n_gx, "gy": n_gy}
    here = {name: lax.axis_index(name) for name in axes}
    gx = here["gx"]
    level, place_x = gx // ROW, lax.rem(gx, ROW)

    def upper(axis):
        return here[axis] < axes[axis] - 1

    def lower(axis):
        return here[axis] > 0

    for ref in (
        xr1, xr2, xr3, zr1, zr2, zr3, xf2r, zf2r, xf3r, zf3r, y1r, y2r, y3r, y4r, dzr, dxr, dxz, bzr, bxr, bxz
    ):
        ref[...] = jnp.zeros(ref.shape, F32)

    barrier = pltpu.get_barrier_semaphore()

    def greet(test, device):
        @pl.when(test)
        def _():
            pl.semaphore_signal(barrier, inc=1, device_id=device, device_id_type=MESH)

    crossing_up = jnp.logical_and(place_x == ROW - 1, upper("gx"))
    crossing_down = jnp.logical_and(place_x == 0, lower("gx"))
    greet(upper("gy"), {"gy": here["gy"] + 1})
    greet(upper("agg"), {"agg": here["agg"] + 1})
    greet(lower("agg"), {"agg": here["agg"] - 1})
    for step in range(1, ROW):
        pl.semaphore_signal(
            barrier, inc=1, device_id={"gx": level * ROW + lax.rem(place_x + step, ROW)}, device_id_type=MESH
        )
    greet(crossing_up, {"gx": gx + 1})
    greet(crossing_down, {"gx": gx - 1})
    greet(level < levels - 1, {"gx": gx + ROW})
    greet(level > 0, {"gx": gx - ROW})

    fetches = [
        pltpu.make_async_copy(source, ref, insem.at[k])
        for k, (source, ref) in enumerate(((vp_in, vp), (r_in, r), (f_in, f), (m_in, mcat)))
    ]
    for fetch in fetches:
        fetch.start()

    def one_copy(message, axis, src, dst, side):
        step = 1 if side == 0 else -1
        return pltpu.make_async_remote_copy(
            src_ref=src[side], dst_ref=dst.at[side],
            send_sem=ssem.at[message, side], recv_sem=rsem.at[message, side],
            device_id={axis: here[axis] + step}, device_id_type=MESH,
        )

    ends = []

    def start(message, axis, src, dst, sides=(0, 1)):
        for side in sides:

            @pl.when(upper(axis) if side == 0 else lower(axis))
            def _(side=side):
                one_copy(message, axis, src, dst, side).start()

            ends.append((message, axis, src, dst, side))

    def arrive(message, axis, src, dst):
        for side in (0, 1):

            @pl.when(lower(axis) if side == 0 else upper(axis))
            def _(side=side):
                one_copy(message, axis, src, dst, side).wait_recv()

    def both(ref):
        return (ref.at[0], ref.at[1])

    lane8, lane16, lane128 = lanes((8, 128)), lanes((16, 128)), lanes((128, 128))
    sub8 = rows((8, 128))
    y_at = lax.rem(rows((128, 128)), 16)

    def comp_of(ref, c):
        return ref[c * 128 : (c + 1) * 128, :]

    def plane(ref, c, j):
        return ref[pl.ds(c * 128 + j, 8, stride=16), :]

    def put_plane(ref, c, j, value):
        ref[pl.ds(c * 128 + j, 8, stride=16), :] = value

    def z_pack(tiles, column, lane):
        packed = jnp.zeros(lane.shape, F32)
        for place, tile in enumerate(tiles):
            packed = jnp.where(lane == place, pltpu.roll(tile, (place - column) % 128, 1), packed)
        return packed

    def z_tiles(ref):
        return [ref[t * 16 : (t + 1) * 16, :] for t in range(24)]

    def x_stage(ref, stage):
        for c in range(3):
            xs[stage, 0, c] = ref[c * 128 + 112 : c * 128 + 128, :]
            xs[stage, 1, c] = ref[c * 128 : c * 128 + 16, :]

    def z_stage(ref, staging):
        tiles = z_tiles(ref)
        staging[0] = z_pack(tiles, 127, lane16)
        staging[1] = z_pack(tiles, 0, lane16)

    def spread(packed, c, lane_at):
        return jnp.concatenate(
            [pltpu.roll(packed, (lane_at - (c * 8 + x)) % 128, 1) for x in range(8)], axis=0
        )

    def around(u, x_low, x_high, z_low, z_high, cut=0):
        total = jnp.concatenate([x_low, u[:112]], axis=0) + jnp.concatenate([u[16:], x_high], axis=0)
        total = total + jnp.where(lane128 == 0, z_low, pltpu.roll(u, 1, 1))
        total = total + jnp.where(lane128 == 127, z_high, pltpu.roll(u, 127, 1))
        total = total + jnp.where(y_at <= cut, 0.0, pltpu.roll(u, 1, 0))
        return total + jnp.where(y_at >= 15 - cut, 0.0, pltpu.roll(u, 127, 0))

    def edges(k, x_got, z_low, z_high):
        value = jnp.where(sub8 == 0, x_got[0, k : k + 1, :], 0.0)
        value = value + jnp.where(sub8 == 7, x_got[1, k : k + 1, :], 0.0)
        value = value + jnp.where(lane8 == 0, pltpu.roll(z_low, (-k) % 128, 1), 0.0)
        return value + jnp.where(lane8 == 127, pltpu.roll(z_high, 127 - k, 1), 0.0)

    def beside(p, k, x_got, z_low, z_high):
        near = jnp.where(sub8 == 0, 0.0, pltpu.roll(p, 1, 0)) + jnp.where(sub8 == 7, 0.0, pltpu.roll(p, 7, 0))
        near = near + jnp.where(lane8 == 0, 0.0, pltpu.roll(p, 1, 1))
        near = near + jnp.where(lane8 == 127, 0.0, pltpu.roll(p, 127, 1))
        return near + edges(k, x_got, z_low, z_high)

    faces = ((0, (15, 14, 13)), (1, (0, 1, 2)))
    mine = ((0, (0, 1, 2)), (1, (15, 14, 13)))

    halves = jnp.where(lax.shift_right_logical(rows((128, 128)), 1) == lane128, 0.125, 0.0)

    def tile_of(ref, t):
        return ref[t * 8 : t * 8 + 8, :]

    def stage_rows(own, staging, at, n):
        for c in range(n):
            a, b, d, e = (tile_of(own, c * 4 + i) for i in range(4))
            up0, up1 = (jnp.where(sub8 < 4, pltpu.roll(v, 4, 0), w) for v, w in ((a, b), (d, e)))
            dn0, dn1 = (jnp.where(sub8 < 4, v, pltpu.roll(w, 4, 0)) for v, w in ((a, b), (d, e)))
            staging[0, at + c] = jnp.where(lane8 < 64, up0, pltpu.roll(up1, 64, 1))
            staging[1, at + c] = jnp.where(lane8 < 64, dn0, pltpu.roll(dn1, 64, 1))

    def unstage_rows(got, at, tile, n):
        for c in range(n):
            for i in range(4):
                low, high = got[0, at + c], got[1, at + c]
                if i >= 2:
                    low, high = pltpu.roll(low, 64, 1), pltpu.roll(high, 64, 1)
                if i % 2 == 0:
                    value = jnp.where(sub8 < 4, high, pltpu.roll(low, 4, 0))
                else:
                    value = jnp.where(sub8 < 4, pltpu.roll(high, 4, 0), low)
                tile[(c * 4 + i) * 8 : (c * 4 + i + 1) * 8, :] = value

    def join(own, tile, pack, staging, n):
        lane = lanes((n * 32, 128))
        pack[...] = jnp.where(lane < 64, own[...], pltpu.roll(tile[...], 64, 1))
        group = lane8 // 4
        sides = [jnp.zeros((8, 128), F32), jnp.zeros((8, 128), F32)]
        for t in range(8 * n):
            value = tile_of(own, t) if t < 4 * n else tile_of(tile, t - 4 * n)
            for side, column in ((0, 60), (1, 0)):
                sides[side] = jnp.where(group == t, pltpu.roll(value, (4 * t - column) % 128, 1), sides[side])
        staging[0], staging[1] = sides

    def assemble(pack, z_got, x_got, xz_got, c, n):
        tiles_ = []
        for place in range(12):
            t = c * 4 + place % 4
            if 4 <= place < 8:
                value, low, high = tile_of(pack, t), z_got[0], z_got[1]
            else:
                side = 0 if place < 4 else 1
                value, low, high = x_got[side, t * 8 : t * 8 + 8, :], xz_got[side, 0], xz_got[side, 1]
            for part, at in ((value, t), (pltpu.roll(value, 64, 1), 4 * n + t)):
                edge = jnp.where(
                    lane8 < 68, pltpu.roll(high, (64 - 4 * at) % 128, 1),
                    jnp.where(lane8 >= 124, pltpu.roll(low, (124 - 4 * at) % 128, 1), 0.0),
                )
                tiles_.append(jnp.where(lane8 < 64, part, edge))
        return jnp.concatenate(tiles_, axis=0)

    def take_turn(turn):
        for way, token in ((1, token_up), (-1, token_down)):
            for n in range(levels):
                if TURNS[n] == turn:

                    @pl.when(level == (n if way == 1 else levels - 1 - n))
                    def _(n=n, way=way, token=token):
                        if n > 0:
                            pl.semaphore_wait(token, 1)
                        if n < levels - 1:
                            pl.semaphore_signal(
                                token, inc=1, device_id={"gx": gx + way * ROW}, device_id_type=MESH
                            )

    fetches[0].wait()
    x_stage(vp, 0)
    z_stage(vp, zs1)
    fetches[1].wait()
    reaction = r[...]
    c_ref[...] = damping / (6.0 + reaction)
    halved = reaction.reshape(4, 2, 16, 128)
    tp[0:64, :] = (halved[:, 0] + halved[:, 1]).reshape(64, 128)
    mean_r = dot(tp[pl.ds(0, 32, stride=2), :] + tp[pl.ds(1, 32, stride=2), :], halves)
    inverse = damping / ((6.0 + 4.0 * mean_r) * 0.25)
    down[...] = inverse
    stage_rows(down, y1s, 5, 1)
    fetches[2].wait()
    for slot, (j, k, _) in faces:
        for c in range(3):
            y1s[slot, c] = plane(vp, c, j)
        y1s[slot, 3] = c_ref[pl.ds(j, 8, stride=16), :]
        y1s[slot, 4] = c_ref[pl.ds(k, 8, stride=16), :]
    fetches[3].wait()

    greeted = ROW - 1
    for test in (
        lower("gy"), upper("agg"), lower("agg"), crossing_up, crossing_down, level < levels - 1, level > 0
    ):
        greeted = greeted + test.astype(jnp.int32)
    pl.semaphore_wait(barrier, greeted)

    @pl.when(lower("gy"))
    def _():
        pl.semaphore_signal(ready, inc=1, device_id={"gy": here["gy"] - 1}, device_id_type=MESH)

    start(X1, "gx", both(xs.at[0]), xr1)
    start(Z1, "agg", both(zs1), zr1)
    start(Y1, "gy", both(y1s), y1r, (1,))

    first = []
    for c in range(3):
        pairs = comp_of(vp, c).reshape(4, 2, 16, 128)
        first.append(((pairs[:, 0] + pairs[:, 1]) * root_half).reshape(64, 128))
    a1 = jnp.concatenate(first, axis=0)
    even = lax.rem(rows((192, 128)), 2) == 0
    a1 = jnp.where(even, a1 + pltpu.roll(a1, 191, 0), pltpu.roll(a1, 1, 0) - a1) * root_half
    out_z, in_z = rows((128, 128)), lane128
    same = lax.shift_right_logical(out_z, 1) == lax.shift_right_logical(in_z, 1)
    minus = jnp.logical_and(lax.rem(out_z, 2) == 1, lax.rem(in_z, 2) == 1)
    pass_z = jnp.where(same, jnp.where(minus, -root_half, root_half), 0.0).astype(F32)
    turned = jnp.concatenate([dot(pass_z, a1, ((1,), (1,))), jnp.zeros((128, 64), F32)], axis=1)
    for t in range(n_gx):
        sendt[t] = turned[t * per : (t + 1) * per, :]

    arrive(X1, "gx", both(xs.at[0]), xr1)
    arrive(Z1, "agg", both(zs1), zr1)
    take_turn(1)
    z_low, z_high = zr1[0], zr1[1]
    for c in range(3):
        u = comp_of(vp, c)
        total = comp_of(f, c) + around(
            u, xr1[0, c], xr1[1, c], spread(z_low, c, 0), spread(z_high, c, 127)
        )
        gb[c * 128 : (c + 1) * 128, :] = total
        u1[c * 128 : (c + 1) * 128, :] = keep * u + c_ref[...] * total
    x_stage(u1, 1)
    start(X2, "gx", both(xs.at[1]), xr2)
    z_stage(u1, zs2)
    start(Z2, "agg", both(zs2), zr2)
    for slot, (j, k, _) in faces:
        for c in range(3):
            y2s[slot, c] = plane(gb, c, j)
            y2s[slot, 3 + c] = plane(f, c, j) + plane(u1, c, k)
    start(Y2, "gy", both(y2s), y2r, (1,))

    arrive(X2, "gx", both(xs.at[1]), xr2)
    arrive(Z2, "agg", both(zs2), zr2)
    take_turn(2)
    z_low, z_high = zr2[0], zr2[1]
    inner = jnp.logical_and(y_at >= 2, y_at <= 13)
    for c in range(3):
        u = comp_of(u1, c)
        total = comp_of(f, c) + around(
            u, xr2[0, c], xr2[1, c], spread(z_low, c, 0), spread(z_high, c, 127), 1
        )
        value = keep * u + c_ref[...] * total
        u2[c * 128 : (c + 1) * 128, :] = value
        uz[c * 128 : (c + 1) * 128, :] = jnp.where(inner, value, 0.0)
    x_stage(uz, 2)
    start(X3, "gx", both(xs.at[2]), xr3)
    z_stage(uz, zs3)
    start(Z3, "agg", both(zs3), zr3)
    for slot, (_, k, _) in faces:
        for c in range(3):
            y3s[slot, c] = plane(u2, c, k)
    start(Y3, "gy", both(y3s), y3r, (1,))

    arrive(X3, "gx", both(xs.at[2]), xr3)
    arrive(Z3, "agg", both(zs3), zr3)
    take_turn(3)
    z3_low, z3_high = zr3[0], zr3[1]
    for c in range(3):
        u = comp_of(uz, c)
        res = (
            comp_of(f, c) - (6.0 + r[...]) * u
            + around(u, xr3[0, c], xr3[1, c], spread(z3_low, c, 0), spread(z3_high, c, 127))
        )
        halved = res.reshape(4, 2, 16, 128)
        tp[c * 64 : (c + 1) * 64, :] = (
            (halved[:, 0] + halved[:, 1]).reshape(64, 128)
        )
    bown[...] = dot(tp[pl.ds(0, 96, stride=2), :] + tp[pl.ds(1, 96, stride=2), :], halves)
    stage_rows(bown, y4s, 0, 3)
    start(Y4, "gy", both(y4s), y4r, (1,))

    @pl.when(upper("gy"))
    def _():
        pl.semaphore_wait(ready, 1)

    for message, src, dst in ((Y1, y1s, y1r), (Y2, y2s, y2r), (Y3, y3s, y3r), (Y4, y4s, y4r)):
        start(message, "gy", both(src), dst, (0,))

    take_turn(4)

    arrive(Y1, "gy", both(y1s), y1r)
    unstage_rows(y1r, 5, dtile, 1)
    join(down, dtile, dpack, dzs, 1)
    start(DZ, "agg", both(dzs), dzr)
    start(DX, "gx", (dpack, dpack), dxr)

    arrive(Y2, "gy", both(y2s), y2r)
    for side, (j, _, _) in mine:
        c0, ch0 = c_ref[pl.ds(j, 8, stride=16), :], y1r[side, 3]
        for c in range(3):
            k = side * 3 + c
            vh = y1r[side, c]
            p1[k * 8 : k * 8 + 8, :] = plane(u1, c, j) + c0 * vh
            p1[48 + k * 8 : 56 + k * 8, :] = keep * vh + ch0 * (y2r[side, c] + plane(vp, c, j))
    xf2s[0, 0:12, :] = p1[pl.ds(7, 12, stride=8), :]
    xf2s[1, 0:12, :] = p1[pl.ds(0, 12, stride=8), :]
    start(XF2, "gx", both(xf2s), xf2r)
    tiles = [p1[k * 8 : k * 8 + 8, :] for k in range(12)]
    zf2s[0] = z_pack(tiles, 127, lane8)
    zf2s[1] = z_pack(tiles, 0, lane8)
    start(ZF2, "agg", both(zf2s), zf2r)

    take_turn(5)

    def send_line(step, carry):
        target = lax.rem(gx + step, n_gx)
        pltpu.make_async_remote_copy(
            src_ref=sendt.at[target], dst_ref=recvt.at[gx],
            send_sem=assem, recv_sem=arsem, device_id={"gx": target}, device_id_type=MESH,
        ).start()
        return carry

    lax.fori_loop(1, n_gx, send_line, 0)

    arrive(Y3, "gy", both(y3s), y3r)
    arrive(XF2, "gx", both(xf2s), xf2r)
    arrive(ZF2, "agg", both(zf2s), zf2r)
    f2_low, f2_high = zf2r[0], zf2r[1]
    for side, (j, j1, _) in mine:
        c0, c1 = c_ref[pl.ds(j, 8, stride=16), :], c_ref[pl.ds(j1, 8, stride=16), :]
        ch0, ch1 = y1r[side, 3], y1r[side, 4]
        for c in range(3):
            k = side * 3 + c
            own, halo = p1[k * 8 : k * 8 + 8, :], p1[48 + k * 8 : 56 + k * 8, :]
            near = beside(own, k, xf2r, f2_low, f2_high)
            p2[k * 8 : k * 8 + 8, :] = keep * own + c0 * (plane(f, c, j) + near + plane(u1, c, j1) + halo)
            p2[48 + k * 8 : 56 + k * 8, :] = plane(u2, c, j1) + c1 * own
            near = beside(halo, 6 + k, xf2r, f2_low, f2_high)
            p2[96 + k * 8 : 104 + k * 8, :] = keep * halo + ch0 * (
                y2r[side, 3 + c] + near + own
            )
            p2[144 + k * 8 : 152 + k * 8, :] = y3r[side, c] + ch1 * halo
    xf3s[0] = p2[pl.ds(7, 24, stride=8), :]
    xf3s[1] = p2[pl.ds(0, 24, stride=8), :]
    start(XF3, "gx", both(xf3s), xf3r)
    tiles = [p2[k * 8 : k * 8 + 8, :] for k in range(24)]
    zf3s[0] = z_pack(tiles, 127, lane8)
    zf3s[1] = z_pack(tiles, 0, lane8)
    start(ZF3, "agg", both(zf3s), zf3r)

    arrive(DZ, "agg", both(dzs), dzr)
    start(DXZ, "gx", (dzr, dzr), dxz)

    arrive(Y4, "gy", both(y4s), y4r)
    unstage_rows(y4r, 0, btile, 3)
    arrive(XF3, "gx", both(xf3s), xf3r)
    arrive(ZF3, "agg", both(zf3s), zf3r)
    f3_low, f3_high = zf3r[0], zf3r[1]
    for side, (j, j1, _) in mine:
        d0 = 6.0 + r[pl.ds(j, 8, stride=16), :]
        d1 = 6.0 + r[pl.ds(j1, 8, stride=16), :]
        ch0, ch1 = y1r[side, 3], y1r[side, 4]
        dh0 = jnp.where(ch0 > 0.0, damping / jnp.where(ch0 > 0.0, ch0, 1.0), 0.0)
        dh1 = jnp.where(ch1 > 0.0, damping / jnp.where(ch1 > 0.0, ch1, 1.0), 0.0)
        for c in range(3):
            k = side * 3 + c
            own0, own1, halo0, halo1 = (p2[n * 48 + k * 8 : n * 48 + k * 8 + 8, :] for n in range(4))
            near = beside(own0, k, xf3r, f3_low, f3_high) + beside(own1, 6 + k, xf3r, f3_low, f3_high)
            ps[k * 8 : k * 8 + 8, :] = near + own1 + halo0 + own0 - d0 * own0 - d1 * own1
            ps[48 + k * 8 : 56 + k * 8, :] = own1
            near = beside(halo0, 12 + k, xf3r, f3_low, f3_high) + beside(halo1, 18 + k, xf3r, f3_low, f3_high)
            ps[96 + k * 8 : 104 + k * 8, :] = near + halo1 + own0 + halo0 - dh0 * halo0 - dh1 * halo1
            ps[144 + k * 8 : 152 + k * 8, :] = halo1
            put_plane(u2, c, j, own0)
            put_plane(u2, c, j1, own1)
    line = dot(ps[pl.ds(0, 96, stride=2), :] + ps[pl.ds(1, 96, stride=2), :], halves)
    for side in (0, 1):
        at0, at1 = ((0, 1), (7, 6))[side]
        to0, to1 = ((7, 6), (0, 1))[side]
        for c in range(3):
            k = (side * 3 + c) * 4
            for ref, row0, row1, base in ((bown, at0, at1, 0), (btile, to0, to1, 48)):
                for row, part in ((row0, k), (row1, 24 + k)):
                    at = pl.ds(c * 32 + row, 4, stride=8)
                    ref[at, :] = ref[at, :] + line[base + part : base + part + 4]
    join(bown, btile, bpack, bzs, 3)
    start(BZ, "agg", both(bzs), bzr)
    start(BX, "gx", (bpack, bpack), bxr)

    arrive(DX, "gx", (dpack, dpack), dxr)
    arrive(DXZ, "gx", (dzr, dzr), dxz)
    cdext[...] = assemble(dpack, dzr, dxr, dxz, 0, 1)

    arrive(BZ, "agg", both(bzs), bzr)
    start(BXZ, "gx", (bzr, bzr), bxz)

    many = n_gx - 1
    lines = pltpu.make_async_remote_copy(
        src_ref=sendt.at[pl.ds(0, many)], dst_ref=recvt.at[pl.ds(0, many)],
        send_sem=assem, recv_sem=arsem, device_id={"gx": lax.rem(gx + 1, n_gx)}, device_id_type=MESH,
    )
    lines.wait_recv()
    lines.wait_send()
    recvt[gx] = sendt[gx]
    for k in range(per):
        got = recvt[:, k, :]
        wide = dot(got[:, 0:192], mcat[...], ((0,), (0,)))
        for c in range(3):
            value = 0.0
            for m in range(4):
                at = (c * 4 + m) * 16
                value = value + wide[at : at + 16, m * 4 * n_gx : (m + 1) * 4 * n_gx]
            comp[c, :, k, :] = value

    arrive(BX, "gx", (bpack, bpack), bxr)
    arrive(BXZ, "gx", (bzr, bzr), bxz)

    y16 = lax.rem(rows((192, 128)), 16)
    fine = lane128 // 2 == rows((128, 128))
    beyond = jnp.logical_or(
        jnp.logical_and(lane128 == 0, rows((128, 128)) == 127),
        jnp.logical_and(lane128 == 127, rows((128, 128)) == 64),
    )
    up = jnp.concatenate([jnp.where(fine, 1.0, 0.0), jnp.where(beyond, 1.0, 0.0)], axis=1).astype(F32)
    none = jnp.zeros((16, 128), F32)
    for c in range(3):
        rhs_c = assemble(bpack, bzr, bxr, bxz, c, 3)
        weight = cdext[...]
        e = weight * rhs_c
        for _ in range(COARSE_SWEEPS - 1):
            near = jnp.concatenate([none, e[:176]], axis=0) + jnp.concatenate([e[16:], none], axis=0)
            near = near + pltpu.roll(e, 1, 1) + pltpu.roll(e, 127, 1)
            near = near + jnp.where(y16 == 0, pltpu.roll(e, 192 - 15, 0), pltpu.roll(e, 1, 0))
            near = near + jnp.where(y16 == 15, pltpu.roll(e, 15, 0), pltpu.roll(e, 191, 0))
            e = keep * e + weight * (rhs_c + 0.25 * near)
        refined = dot(e[48:144], up)
        eu[c * 96 : (c + 1) * 96, :] = refined[:, 0:128]
        for ref, part in ((cf, refined[:, 0:128]), (cz, refined[:, 128:256])):
            main = part.reshape(6, 16, 128)[:, 0:8].reshape(48, 128)
            ref[pl.ds(c * 96, 48, stride=2), :] = main
            ref[pl.ds(c * 96 + 1, 48, stride=2), :] = main
        for side, row in ((0, 15), (1, 8)):
            line_ = eu[pl.ds(c * 96 + 16 + row, 4, stride=16), :]
            at = (side * 3 + c) * 8
            ph[pl.ds(at, 4, stride=2), :] = line_
            ph[pl.ds(at + 1, 4, stride=2), :] = line_

    def doubled(ref, c):
        value = ref[c * 96 + 16 : c * 96 + 80, :].reshape(4, 1, 16, 128)
        return jnp.broadcast_to(value, (4, 2, 16, 128)).reshape(128, 128)

    for c in range(3):
        w = comp_of(u2, c) + doubled(cf, c)
        outer = doubled(cz, c)
        total = comp_of(f, c) + around(
            w,
            xr3[0, c] + cf[c * 96 : c * 96 + 16, :],
            xr3[1, c] + cf[c * 96 + 80 : c * 96 + 96, :],
            spread(z3_low, c, 0) + outer,
            spread(z3_high, c, 127) + outer,
        )
        vel[c * 128 : (c + 1) * 128, :] = keep * w + c_ref[...] * total
    for side, (j, j1, _) in mine:
        c0, c1 = c_ref[pl.ds(j, 8, stride=16), :], c_ref[pl.ds(j1, 8, stride=16), :]
        for c in range(3):
            k = side * 3 + c
            more = edges(k, xf3r, f3_low, f3_high)
            more = more + p2[96 + k * 8 : 104 + k * 8, :] + ph[k * 8 : k * 8 + 8, :]
            put_plane(vel, c, j, plane(vel, c, j) + c0 * more)
            more = edges(6 + k, xf3r, f3_low, f3_high)
            put_plane(vel, c, j1, plane(vel, c, j1) + c1 * more)

    for message, axis, src, dst, side in ends:

        @pl.when(upper(axis) if side == 0 else lower(axis))
        def _(args=(message, axis, src, dst, side)):
            one_copy(*args).wait_send()


def on_device(sizes, velocity_prev, forcing, reaction):
    n_agg, n_gx, n_gy = sizes
    per = 128 // n_gx

    def v(*shape):
        return pltpu.VMEM(shape, F32)

    scratch = [
        v(384, 128), v(384, 128), v(128, 128), v(n_gx, 16 * n_gx),
        v(128, 128), v(384, 128), v(384, 128), v(384, 128), v(384, 128), v(192, 128),
        v(n_gx, per, 256), v(n_gx, per, 256),
        v(3, 2, 3, 16, 128), v(2, 3, 16, 128), v(2, 3, 16, 128), v(2, 3, 16, 128),
    ]
    scratch += [v(2, 16, 128)] * 6
    scratch += [v(96, 128), v(192, 128), v(192, 128)]
    scratch += [v(2, 16, 128)] * 2 + [v(2, 8, 128)] * 2 + [v(2, 24, 128)] * 2 + [v(2, 8, 128)] * 2
    scratch += [v(2, 6, 8, 128)] * 4 + [v(2, 3, 8, 128)] * 4
    for n in (1, 3):
        scratch += [v(n * 32, 128)] * 3 + [v(2, n * 32, 128), v(2, 8, 128), v(2, 8, 128), v(2, 2, 8, 128)]
    scratch += [v(192, 128), v(288, 128), v(288, 128), v(288, 128), v(48, 128)]
    dma = pltpu.SemaphoreType.DMA
    scratch += [dma((4,)), dma((COUNT, 2)), dma((COUNT, 2)), dma, dma]
    scratch += [pltpu.SemaphoreType.REGULAR] * 3
    vmem = pl.BlockSpec(memory_space=pltpu.VMEM)
    velocity, compressed = pl.pallas_call(
        functools.partial(kernel, sizes),
        out_shape=(
            jax.ShapeDtypeStruct((384, 128), F32),
            jax.ShapeDtypeStruct((3, 16, per, 4 * n_gx), F32),
        ),
        in_specs=[pl.BlockSpec(memory_space=pltpu.HBM)] * 4,
        out_specs=(vmem, vmem),
        scratch_shapes=scratch,
        compiler_params=pltpu.CompilerParams(collective_id=0, has_side_effects=True),
        name="vcycle",
    )(
        velocity_prev.reshape(384, 128), forcing.reshape(384, 128), reaction.reshape(128, 128),
        jnp.asarray(haar_matrix(n_gx)),
    )
    return velocity.reshape(3, 8, 16, 128), compressed


def solution(mesh):
    placed = (P(None, "gx", "gy", "agg"), P(None, "gx", "gy", "agg"), P("gx", "gy", "agg"))
    sizes = tuple(mesh.shape[name] for name in ("agg", "gx", "gy"))
    return jax.shard_map(
        functools.partial(on_device, sizes),
        mesh=mesh,
        in_specs=placed,
        out_specs=(P(None, "gx", "gy", "agg"), P(None, "gy", ("agg", "gx"), None)),
        check_vma=False,
    )
```

```python
import functools

import jax
import jax.numpy as jnp
import numpy as np
from jax import lax
from jax.experimental import pallas as pl
from jax.experimental.pallas import tpu as pltpu
from jax.sharding import PartitionSpec as P

SWEEPS = 2
COARSE_SWEEPS = 4
LX = 5
damping = 0.8
keep = 1.0 - damping
root_half = 0.7071067811865476
MESH = pl.DeviceIdType.MESH
F32 = jnp.float32

X1, Z1, X2, Z2, X3, Z3, XF2, ZF2, XF3, ZF3, DZ, DX, DXZ, BZ, BX, BXZ, Y1, Y2, Y3, Y4, COUNT = range(21)
ROW = 4
TURNS = (1, 1, 2, 2, 3, 3, 4, 5)

def haar_matrix(devices):
    size = 4 * devices
    approx = np.eye(size)
    details = []
    for _ in range(LX - 1):
        even, odd = approx[:, 0::2], approx[:, 1::2]
        approx, detail = (even + odd) * root_half, (even - odd) * root_half
        details.append(detail)
    whole = np.concatenate([approx] + details[::-1], axis=1)
    parts = whole.reshape(devices, 4, size)
    return np.concatenate([parts[:, m] for m in range(4)], axis=1).astype(np.float32)


def dot(a, b, dims=((1,), (0,))):
    return lax.dot_general(
        a, b, (dims, ((), ())), precision=lax.Precision.HIGHEST, preferred_element_type=F32
    )


def lanes(shape):
    return lax.broadcasted_iota(jnp.int32, shape, len(shape) - 1)


def rows(shape):
    return lax.broadcasted_iota(jnp.int32, shape, len(shape) - 2)


def kernel(
    sizes, vp_in, f_in, r_in, m_in, vel, comp,
    vp, f, r, mcat, c_ref, u1, u2, uz, gb, tp, sendt, recvt,
    xs, xr1, xr2, xr3, zs1, zr1, zs2, zr2, zs3, zr3,
    p1, p2, ps, xf2s, xf2r, zf2s, zf2r, xf3s, xf3r, zf3s, zf3r,
    y1s, y1r, y2s, y2r, y3s, y3r, y4s, y4r,
    down, dtile, dpack, dxr, dzs, dzr, dxz, bown, btile, bpack, bxr, bzs, bzr, bxz,
    cdext, cf, cz, eu, ph,
    insem, ssem, rsem, assem, arsem, ready, token_up, token_down,
):
    n_agg, n_gx, n_gy = sizes
    per = 128 // n_gx
    levels = n_gx // ROW
    axes = {"agg": n_agg, "gx": n_gx, "gy": n_gy}
    here = {name: lax.axis_index(name) for name in axes}
    gx = here["gx"]
    level, place_x = gx // ROW, lax.rem(gx, ROW)

    def upper(axis):
        return here[axis] < axes[axis] - 1

    def lower(axis):
        return here[axis] > 0

    for ref in (
        xr1, xr2, xr3, zr1, zr2, zr3, xf2r, zf2r, xf3r, zf3r, y1r, y2r, y3r, y4r, dzr, dxr, dxz, bzr, bxr, bxz
    ):
        ref[...] = jnp.zeros(ref.shape, F32)

    barrier = pltpu.get_barrier_semaphore()

    def greet(test, device):
        @pl.when(test)
        def _():
            pl.semaphore_signal(barrier, inc=1, device_id=device, device_id_type=MESH)

    crossing_up = jnp.logical_and(place_x == ROW - 1, upper("gx"))
    crossing_down = jnp.logical_and(place_x == 0, lower("gx"))
    greet(upper("gy"), {"gy": here["gy"] + 1})
    greet(upper("agg"), {"agg": here["agg"] + 1})
    greet(lower("agg"), {"agg": here["agg"] - 1})
    for step in range(1, ROW):
        pl.semaphore_signal(
            barrier, inc=1, device_id={"gx": level * ROW + lax.rem(place_x + step, ROW)}, device_id_type=MESH
        )
    greet(crossing_up, {"gx": gx + 1})
    greet(crossing_down, {"gx": gx - 1})
    greet(level < levels - 1, {"gx": gx + ROW})
    greet(level > 0, {"gx": gx - ROW})

    fetches = [
        pltpu.make_async_copy(source, ref, insem.at[k])
        for k, (source, ref) in enumerate(((vp_in, vp), (r_in, r), (f_in, f), (m_in, mcat)))
    ]
    for fetch in fetches:
        fetch.start()

    def one_copy(message, axis, src, dst, side):
        step = 1 if side == 0 else -1
        return pltpu.make_async_remote_copy(
            src_ref=src[side], dst_ref=dst.at[side],
            send_sem=ssem.at[message, side], recv_sem=rsem.at[message, side],
            device_id={axis: here[axis] + step}, device_id_type=MESH,
        )

    ends = []

    def start(message, axis, src, dst, sides=(0, 1)):
        for side in sides:

            @pl.when(upper(axis) if side == 0 else lower(axis))
            def _(side=side):
                one_copy(message, axis, src, dst, side).start()

            ends.append((message, axis, src, dst, side))

    def arrive(message, axis, src, dst):
        for side in (0, 1):

            @pl.when(lower(axis) if side == 0 else upper(axis))
            def _(side=side):
                one_copy(message, axis, src, dst, side).wait_recv()

    def both(ref):
        return (ref.at[0], ref.at[1])

    lane8, lane16, lane128 = lanes((8, 128)), lanes((16, 128)), lanes((128, 128))
    sub8 = rows((8, 128))
    y_at = lax.rem(rows((128, 128)), 16)

    def comp_of(ref, c):
        return ref[c * 128 : (c + 1) * 128, :]

    def plane(ref, c, j):
        return ref[pl.ds(c * 128 + j, 8, stride=16), :]

    def put_plane(ref, c, j, value):
        ref[pl.ds(c * 128 + j, 8, stride=16), :] = value

    def z_pack(tiles, column, lane):
        packed = jnp.zeros(lane.shape, F32)
        for place, tile in enumerate(tiles):
            packed = jnp.where(lane == place, pltpu.roll(tile, (place - column) % 128, 1), packed)
        return packed

    def z_tiles(ref):
        return [ref[t * 16 : (t + 1) * 16, :] for t in range(24)]

    def x_stage(ref, stage):
        for c in range(3):
            xs[stage, 0, c] = ref[c * 128 + 112 : c * 128 + 128, :]
            xs[stage, 1, c] = ref[c * 128 : c * 128 + 16, :]

    def z_stage(ref, staging):
        tiles = z_tiles(ref)
        staging[0] = z_pack(tiles, 127, lane16)
        staging[1] = z_pack(tiles, 0, lane16)

    def spread(packed, c, lane_at):
        return jnp.concatenate(
            [pltpu.roll(packed, (lane_at - (c * 8 + x)) % 128, 1) for x in range(8)], axis=0
        )

    def around(u, x_low, x_high, z_low, z_high, cut=0):
        total = jnp.concatenate([x_low, u[:112]], axis=0) + jnp.concatenate([u[16:], x_high], axis=0)
        total = total + jnp.where(lane128 == 0, z_low, pltpu.roll(u, 1, 1))
        total = total + jnp.where(lane128 == 127, z_high, pltpu.roll(u, 127, 1))
        total = total + jnp.where(y_at <= cut, 0.0, pltpu.roll(u, 1, 0))
        return total + jnp.where(y_at >= 15 - cut, 0.0, pltpu.roll(u, 127, 0))

    def edges(k, x_got, z_low, z_high):
        value = jnp.where(sub8 == 0, x_got[0, k : k + 1, :], 0.0)
        value = value + jnp.where(sub8 == 7, x_got[1, k : k + 1, :], 0.0)
        value = value + jnp.where(lane8 == 0, pltpu.roll(z_low, (-k) % 128, 1), 0.0)
        return value + jnp.where(lane8 == 127, pltpu.roll(z_high, 127 - k, 1), 0.0)

    def beside(p, k, x_got, z_low, z_high):
        near = jnp.where(sub8 == 0, 0.0, pltpu.roll(p, 1, 0)) + jnp.where(sub8 == 7, 0.0, pltpu.roll(p, 7, 0))
        near = near + jnp.where(lane8 == 0, 0.0, pltpu.roll(p, 1, 1))
        near = near + jnp.where(lane8 == 127, 0.0, pltpu.roll(p, 127, 1))
        return near + edges(k, x_got, z_low, z_high)

    faces = ((0, (15, 14, 13)), (1, (0, 1, 2)))
    mine = ((0, (0, 1, 2)), (1, (15, 14, 13)))

    halves = jnp.where(lax.shift_right_logical(rows((128, 128)), 1) == lane128, 0.125, 0.0)

    def tile_of(ref, t):
        return ref[t * 8 : t * 8 + 8, :]

    def stage_rows(own, staging, at, n):
        for c in range(n):
            a, b, d, e = (tile_of(own, c * 4 + i) for i in range(4))
            up0, up1 = (jnp.where(sub8 < 4, pltpu.roll(v, 4, 0), w) for v, w in ((a, b), (d, e)))
            dn0, dn1 = (jnp.where(sub8 < 4, v, pltpu.roll(w, 4, 0)) for v, w in ((a, b), (d, e)))
            staging[0, at + c] = jnp.where(lane8 < 64, up0, pltpu.roll(up1, 64, 1))
            staging[1, at + c] = jnp.where(lane8 < 64, dn0, pltpu.roll(dn1, 64, 1))

    def unstage_rows(got, at, tile, n):
        for c in range(n):
            for i in range(4):
                low, high = got[0, at + c], got[1, at + c]
                if i >= 2:
                    low, high = pltpu.roll(low, 64, 1), pltpu.roll(high, 64, 1)
                if i % 2 == 0:
                    value = jnp.where(sub8 < 4, high, pltpu.roll(low, 4, 0))
                else:
                    value = jnp.where(sub8 < 4, pltpu.roll(high, 4, 0), low)
                tile[(c * 4 + i) * 8 : (c * 4 + i + 1) * 8, :] = value

    def join(own, tile, pack, staging, n):
        lane = lanes((n * 32, 128))
        pack[...] = jnp.where(lane < 64, own[...], pltpu.roll(tile[...], 64, 1))
        group = lane8 // 4
        sides = [jnp.zeros((8, 128), F32), jnp.zeros((8, 128), F32)]
        for t in range(8 * n):
            value = tile_of(own, t) if t < 4 * n else tile_of(tile, t - 4 * n)
            for side, column in ((0, 60), (1, 0)):
                sides[side] = jnp.where(group == t, pltpu.roll(value, (4 * t - column) % 128, 1), sides[side])
        staging[0], staging[1] = sides

    def assemble(pack, z_got, x_got, xz_got, c, n):
        tiles_ = []
        for place in range(12):
            t = c * 4 + place % 4
            if 4 <= place < 8:
                value, low, high = tile_of(pack, t), z_got[0], z_got[1]
            else:
                side = 0 if place < 4 else 1
                value, low, high = x_got[side, t * 8 : t * 8 + 8, :], xz_got[side, 0], xz_got[side, 1]
            for part, at in ((value, t), (pltpu.roll(value, 64, 1), 4 * n + t)):
                edge = jnp.where(
                    lane8 < 68, pltpu.roll(high, (64 - 4 * at) % 128, 1),
                    jnp.where(lane8 >= 124, pltpu.roll(low, (124 - 4 * at) % 128, 1), 0.0),
                )
                tiles_.append(jnp.where(lane8 < 64, part, edge))
        return jnp.concatenate(tiles_, axis=0)

    def take_turn(turn):
        for way, token in ((1, token_up), (-1, token_down)):
            for n in range(levels):
                if TURNS[n] == turn:

                    @pl.when(level == (n if way == 1 else levels - 1 - n))
                    def _(n=n, way=way, token=token):
                        if n > 0:
                            pl.semaphore_wait(token, 1)
                        if n < levels - 1:
                            pl.semaphore_signal(
                                token, inc=1, device_id={"gx": gx + way * ROW}, device_id_type=MESH
                            )

    fetches[0].wait()
    x_stage(vp, 0)
    greeted = ROW - 1
    for test in (
        lower("gy"), upper("agg"), lower("agg"), crossing_up, crossing_down, level < levels - 1, level > 0
    ):
        greeted = greeted + test.astype(jnp.int32)
    pl.semaphore_wait(barrier, greeted)

    @pl.when(lower("gy"))
    def _():
        pl.semaphore_signal(ready, inc=1, device_id={"gy": here["gy"] - 1}, device_id_type=MESH)

    start(X1, "gx", both(xs.at[0]), xr1)
    z_stage(vp, zs1)
    start(Z1, "agg", both(zs1), zr1)

    fetches[1].wait()
    reaction = r[...]
    c_ref[...] = damping / (6.0 + reaction)
    halved = reaction.reshape(4, 2, 16, 128)
    tp[0:64, :] = (halved[:, 0] + halved[:, 1]).reshape(64, 128)
    mean_r = dot(tp[pl.ds(0, 32, stride=2), :] + tp[pl.ds(1, 32, stride=2), :], halves)
    inverse = damping / ((6.0 + 4.0 * mean_r) * 0.25)
    down[...] = inverse
    stage_rows(down, y1s, 5, 1)
    for slot, (j, k, _) in faces:
        for c in range(3):
            y1s[slot, c] = plane(vp, c, j)
        y1s[slot, 3] = c_ref[pl.ds(j, 8, stride=16), :]
        y1s[slot, 4] = c_ref[pl.ds(k, 8, stride=16), :]
    start(Y1, "gy", both(y1s), y1r, (1,))
    fetches[2].wait()
    fetches[3].wait()

    first = []
    for c in range(3):
        pairs = comp_of(vp, c).reshape(4, 2, 16, 128)
        first.append(((pairs[:, 0] + pairs[:, 1]) * root_half).reshape(64, 128))
    a1 = jnp.concatenate(first, axis=0)
    even = lax.rem(rows((192, 128)), 2) == 0
    a1 = jnp.where(even, a1 + pltpu.roll(a1, 191, 0), pltpu.roll(a1, 1, 0) - a1) * root_half
    out_z, in_z = rows((128, 128)), lane128
    same = lax.shift_right_logical(out_z, 1) == lax.shift_right_logical(in_z, 1)
    minus = jnp.logical_and(lax.rem(out_z, 2) == 1, lax.rem(in_z, 2) == 1)
    pass_z = jnp.where(same, jnp.where(minus, -root_half, root_half), 0.0).astype(F32)
    turned = jnp.concatenate([dot(pass_z, a1, ((1,), (1,))), jnp.zeros((128, 64), F32)], axis=1)
    for t in range(n_gx):
        sendt[t] = turned[t * per : (t + 1) * per, :]

    arrive(X1, "gx", both(xs.at[0]), xr1)
    arrive(Z1, "agg", both(zs1), zr1)
    take_turn(1)
    z_low, z_high = zr1[0], zr1[1]
    for c in range(3):
        u = comp_of(vp, c)
        total = comp_of(f, c) + around(
            u, xr1[0, c], xr1[1, c], spread(z_low, c, 0), spread(z_high, c, 127)
        )
        gb[c * 128 : (c + 1) * 128, :] = total
        u1[c * 128 : (c + 1) * 128, :] = keep * u + c_ref[...] * total
    x_stage(u1, 1)
    start(X2, "gx", both(xs.at[1]), xr2)
    z_stage(u1, zs2)
    start(Z2, "agg", both(zs2), zr2)
    for slot, (j, k, _) in faces:
        for c in range(3):
            y2s[slot, c] = plane(gb, c, j)
            y2s[slot, 3 + c] = plane(f, c, j) + plane(u1, c, k)
    start(Y2, "gy", both(y2s), y2r, (1,))

    arrive(X2, "gx", both(xs.at[1]), xr2)
    arrive(Z2, "agg", both(zs2), zr2)
    take_turn(2)
    z_low, z_high = zr2[0], zr2[1]
    inner = jnp.logical_and(y_at >= 2, y_at <= 13)
    for c in range(3):
        u = comp_of(u1, c)
        total = comp_of(f, c) + around(
            u, xr2[0, c], xr2[1, c], spread(z_low, c, 0), spread(z_high, c, 127), 1
        )
        value = keep * u + c_ref[...] * total
        u2[c * 128 : (c + 1) * 128, :] = value
        uz[c * 128 : (c + 1) * 128, :] = jnp.where(inner, value, 0.0)
    x_stage(uz, 2)
    start(X3, "gx", both(xs.at[2]), xr3)
    z_stage(uz, zs3)
    start(Z3, "agg", both(zs3), zr3)
    for slot, (_, k, _) in faces:
        for c in range(3):
            y3s[slot, c] = plane(u2, c, k)
    start(Y3, "gy", both(y3s), y3r, (1,))

    @pl.when(upper("gy"))
    def _():
        pl.semaphore_wait(ready, 1)

    for message, src, dst in ((Y1, y1s, y1r), (Y2, y2s, y2r), (Y3, y3s, y3r)):
        start(message, "gy", both(src), dst, (0,))

    arrive(X3, "gx", both(xs.at[2]), xr3)
    arrive(Z3, "agg", both(zs3), zr3)
    take_turn(3)
    z3_low, z3_high = zr3[0], zr3[1]
    for c in range(3):
        u = comp_of(uz, c)
        res = (
            comp_of(f, c) - (6.0 + r[...]) * u
            + around(u, xr3[0, c], xr3[1, c], spread(z3_low, c, 0), spread(z3_high, c, 127))
        )
        halved = res.reshape(4, 2, 16, 128)
        tp[c * 64 : (c + 1) * 64, :] = (
            (halved[:, 0] + halved[:, 1]).reshape(64, 128)
        )
    bown[...] = dot(tp[pl.ds(0, 96, stride=2), :] + tp[pl.ds(1, 96, stride=2), :], halves)
    stage_rows(bown, y4s, 0, 3)
    start(Y4, "gy", both(y4s), y4r)

    take_turn(4)

    arrive(Y1, "gy", both(y1s), y1r)
    unstage_rows(y1r, 5, dtile, 1)
    join(down, dtile, dpack, dzs, 1)
    start(DZ, "agg", both(dzs), dzr)
    start(DX, "gx", (dpack, dpack), dxr)

    arrive(Y2, "gy", both(y2s), y2r)
    for side, (j, _, _) in mine:
        c0, ch0 = c_ref[pl.ds(j, 8, stride=16), :], y1r[side, 3]
        for c in range(3):
            k = side * 3 + c
            vh = y1r[side, c]
            p1[k * 8 : k * 8 + 8, :] = plane(u1, c, j) + c0 * vh
            p1[48 + k * 8 : 56 + k * 8, :] = keep * vh + ch0 * (y2r[side, c] + plane(vp, c, j))
    xf2s[0, 0:12, :] = p1[pl.ds(7, 12, stride=8), :]
    xf2s[1, 0:12, :] = p1[pl.ds(0, 12, stride=8), :]
    start(XF2, "gx", both(xf2s), xf2r)
    tiles = [p1[k * 8 : k * 8 + 8, :] for k in range(12)]
    zf2s[0] = z_pack(tiles, 127, lane8)
    zf2s[1] = z_pack(tiles, 0, lane8)
    start(ZF2, "agg", both(zf2s), zf2r)

    take_turn(5)

    def send_line(step, carry):
        target = lax.rem(gx + step, n_gx)
        pltpu.make_async_remote_copy(
            src_ref=sendt.at[target], dst_ref=recvt.at[gx],
            send_sem=assem, recv_sem=arsem, device_id={"gx": target}, device_id_type=MESH,
        ).start()
        return carry

    lax.fori_loop(1, n_gx, send_line, 0)

    arrive(Y3, "gy", both(y3s), y3r)
    arrive(XF2, "gx", both(xf2s), xf2r)
    arrive(ZF2, "agg", both(zf2s), zf2r)
    f2_low, f2_high = zf2r[0], zf2r[1]
    for side, (j, j1, _) in mine:
        c0, c1 = c_ref[pl.ds(j, 8, stride=16), :], c_ref[pl.ds(j1, 8, stride=16), :]
        ch0, ch1 = y1r[side, 3], y1r[side, 4]
        for c in range(3):
            k = side * 3 + c
            own, halo = p1[k * 8 : k * 8 + 8, :], p1[48 + k * 8 : 56 + k * 8, :]
            near = beside(own, k, xf2r, f2_low, f2_high)
            p2[k * 8 : k * 8 + 8, :] = keep * own + c0 * (plane(f, c, j) + near + plane(u1, c, j1) + halo)
            p2[48 + k * 8 : 56 + k * 8, :] = plane(u2, c, j1) + c1 * own
            near = beside(halo, 6 + k, xf2r, f2_low, f2_high)
            p2[96 + k * 8 : 104 + k * 8, :] = keep * halo + ch0 * (
                y2r[side, 3 + c] + near + own
            )
            p2[144 + k * 8 : 152 + k * 8, :] = y3r[side, c] + ch1 * halo
    xf3s[0] = p2[pl.ds(7, 24, stride=8), :]
    xf3s[1] = p2[pl.ds(0, 24, stride=8), :]
    start(XF3, "gx", both(xf3s), xf3r)
    tiles = [p2[k * 8 : k * 8 + 8, :] for k in range(24)]
    zf3s[0] = z_pack(tiles, 127, lane8)
    zf3s[1] = z_pack(tiles, 0, lane8)
    start(ZF3, "agg", both(zf3s), zf3r)

    arrive(DZ, "agg", both(dzs), dzr)
    start(DXZ, "gx", (dzr, dzr), dxz)

    arrive(Y4, "gy", both(y4s), y4r)
    unstage_rows(y4r, 0, btile, 3)
    arrive(XF3, "gx", both(xf3s), xf3r)
    arrive(ZF3, "agg", both(zf3s), zf3r)
    f3_low, f3_high = zf3r[0], zf3r[1]
    for side, (j, j1, _) in mine:
        d0 = 6.0 + r[pl.ds(j, 8, stride=16), :]
        d1 = 6.0 + r[pl.ds(j1, 8, stride=16), :]
        ch0, ch1 = y1r[side, 3], y1r[side, 4]
        dh0 = jnp.where(ch0 > 0.0, damping / jnp.where(ch0 > 0.0, ch0, 1.0), 0.0)
        dh1 = jnp.where(ch1 > 0.0, damping / jnp.where(ch1 > 0.0, ch1, 1.0), 0.0)
        for c in range(3):
            k = side * 3 + c
            own0, own1, halo0, halo1 = (p2[n * 48 + k * 8 : n * 48 + k * 8 + 8, :] for n in range(4))
            near = beside(own0, k, xf3r, f3_low, f3_high) + beside(own1, 6 + k, xf3r, f3_low, f3_high)
            ps[k * 8 : k * 8 + 8, :] = near + own1 + halo0 + own0 - d0 * own0 - d1 * own1
            ps[48 + k * 8 : 56 + k * 8, :] = own1
            near = beside(halo0, 12 + k, xf3r, f3_low, f3_high) + beside(halo1, 18 + k, xf3r, f3_low, f3_high)
            ps[96 + k * 8 : 104 + k * 8, :] = near + halo1 + own0 + halo0 - dh0 * halo0 - dh1 * halo1
            ps[144 + k * 8 : 152 + k * 8, :] = halo1
            put_plane(u2, c, j, own0)
            put_plane(u2, c, j1, own1)
    line = dot(ps[pl.ds(0, 96, stride=2), :] + ps[pl.ds(1, 96, stride=2), :], halves)
    for side in (0, 1):
        at0, at1 = ((0, 1), (7, 6))[side]
        to0, to1 = ((7, 6), (0, 1))[side]
        for c in range(3):
            k = (side * 3 + c) * 4
            for ref, row0, row1, base in ((bown, at0, at1, 0), (btile, to0, to1, 48)):
                for row, part in ((row0, k), (row1, 24 + k)):
                    at = pl.ds(c * 32 + row, 4, stride=8)
                    ref[at, :] = ref[at, :] + line[base + part : base + part + 4]
    join(bown, btile, bpack, bzs, 3)
    start(BZ, "agg", both(bzs), bzr)
    start(BX, "gx", (bpack, bpack), bxr)

    arrive(DX, "gx", (dpack, dpack), dxr)
    arrive(DXZ, "gx", (dzr, dzr), dxz)
    cdext[...] = assemble(dpack, dzr, dxr, dxz, 0, 1)

    arrive(BZ, "agg", both(bzs), bzr)
    start(BXZ, "gx", (bzr, bzr), bxz)

    many = n_gx - 1
    lines = pltpu.make_async_remote_copy(
        src_ref=sendt.at[pl.ds(0, many)], dst_ref=recvt.at[pl.ds(0, many)],
        send_sem=assem, recv_sem=arsem, device_id={"gx": lax.rem(gx + 1, n_gx)}, device_id_type=MESH,
    )
    lines.wait_recv()
    lines.wait_send()
    recvt[gx] = sendt[gx]
    for k in range(per):
        got = recvt[:, k, :]
        wide = dot(got[:, 0:192], mcat[...], ((0,), (0,)))
        for c in range(3):
            value = 0.0
            for m in range(4):
                at = (c * 4 + m) * 16
                value = value + wide[at : at + 16, m * 4 * n_gx : (m + 1) * 4 * n_gx]
            comp[c, :, k, :] = value

    arrive(BX, "gx", (bpack, bpack), bxr)
    arrive(BXZ, "gx", (bzr, bzr), bxz)

    y16 = lax.rem(rows((192, 128)), 16)
    fine = lane128 // 2 == rows((128, 128))
    beyond = jnp.logical_or(
        jnp.logical_and(lane128 == 0, rows((128, 128)) == 127),
        jnp.logical_and(lane128 == 127, rows((128, 128)) == 64),
    )
    up = jnp.concatenate([jnp.where(fine, 1.0, 0.0), jnp.where(beyond, 1.0, 0.0)], axis=1).astype(F32)
    none = jnp.zeros((16, 128), F32)
    for c in range(3):
        rhs_c = assemble(bpack, bzr, bxr, bxz, c, 3)
        weight = cdext[...]
        e = weight * rhs_c
        for _ in range(COARSE_SWEEPS - 1):
            near = jnp.concatenate([none, e[:176]], axis=0) + jnp.concatenate([e[16:], none], axis=0)
            near = near + pltpu.roll(e, 1, 1) + pltpu.roll(e, 127, 1)
            near = near + jnp.where(y16 == 0, pltpu.roll(e, 192 - 15, 0), pltpu.roll(e, 1, 0))
            near = near + jnp.where(y16 == 15, pltpu.roll(e, 15, 0), pltpu.roll(e, 191, 0))
            e = keep * e + weight * (rhs_c + 0.25 * near)
        refined = dot(e[48:144], up)
        eu[c * 96 : (c + 1) * 96, :] = refined[:, 0:128]
        for ref, part in ((cf, refined[:, 0:128]), (cz, refined[:, 128:256])):
            main = part.reshape(6, 16, 128)[:, 0:8].reshape(48, 128)
            ref[pl.ds(c * 96, 48, stride=2), :] = main
            ref[pl.ds(c * 96 + 1, 48, stride=2), :] = main
        for side, row in ((0, 15), (1, 8)):
            line_ = eu[pl.ds(c * 96 + 16 + row, 4, stride=16), :]
            at = (side * 3 + c) * 8
            ph[pl.ds(at, 4, stride=2), :] = line_
            ph[pl.ds(at + 1, 4, stride=2), :] = line_

    def doubled(ref, c):
        value = ref[c * 96 + 16 : c * 96 + 80, :].reshape(4, 1, 16, 128)
        return jnp.broadcast_to(value, (4, 2, 16, 128)).reshape(128, 128)

    for c in range(3):
        w = comp_of(u2, c) + doubled(cf, c)
        outer = doubled(cz, c)
        total = comp_of(f, c) + around(
            w,
            xr3[0, c] + cf[c * 96 : c * 96 + 16, :],
            xr3[1, c] + cf[c * 96 + 80 : c * 96 + 96, :],
            spread(z3_low, c, 0) + outer,
            spread(z3_high, c, 127) + outer,
        )
        vel[c * 128 : (c + 1) * 128, :] = keep * w + c_ref[...] * total
    for side, (j, j1, _) in mine:
        c0, c1 = c_ref[pl.ds(j, 8, stride=16), :], c_ref[pl.ds(j1, 8, stride=16), :]
        for c in range(3):
            k = side * 3 + c
            more = edges(k, xf3r, f3_low, f3_high)
            more = more + p2[96 + k * 8 : 104 + k * 8, :] + ph[k * 8 : k * 8 + 8, :]
            put_plane(vel, c, j, plane(vel, c, j) + c0 * more)
            more = edges(6 + k, xf3r, f3_low, f3_high)
            put_plane(vel, c, j1, plane(vel, c, j1) + c1 * more)

    for message, axis, src, dst, side in ends:

        @pl.when(upper(axis) if side == 0 else lower(axis))
        def _(args=(message, axis, src, dst, side)):
            one_copy(*args).wait_send()


def put_kernel(velocity, compressed, velocity_out, compressed_out, sem):
    copies = [
        pltpu.make_async_copy(velocity, velocity_out, sem.at[0]),
        pltpu.make_async_copy(compressed, compressed_out, sem.at[1]),
    ]
    for copy in copies:
        copy.start()
    for copy in copies:
        copy.wait()


def on_device(sizes, velocity_prev, forcing, reaction):
    n_agg, n_gx, n_gy = sizes
    per = 128 // n_gx

    def v(*shape):
        return pltpu.VMEM(shape, F32)

    scratch = [
        v(384, 128), v(384, 128), v(128, 128), v(n_gx, 16 * n_gx),
        v(128, 128), v(384, 128), v(384, 128), v(384, 128), v(384, 128), v(192, 128),
        v(n_gx, per, 256), v(n_gx, per, 256),
        v(3, 2, 3, 16, 128), v(2, 3, 16, 128), v(2, 3, 16, 128), v(2, 3, 16, 128),
    ]
    scratch += [v(2, 16, 128)] * 6
    scratch += [v(96, 128), v(192, 128), v(192, 128)]
    scratch += [v(2, 16, 128)] * 2 + [v(2, 8, 128)] * 2 + [v(2, 24, 128)] * 2 + [v(2, 8, 128)] * 2
    scratch += [v(2, 6, 8, 128)] * 4 + [v(2, 3, 8, 128)] * 4
    for n in (1, 3):
        scratch += [v(n * 32, 128)] * 3 + [v(2, n * 32, 128), v(2, 8, 128), v(2, 8, 128), v(2, 2, 8, 128)]
    scratch += [v(192, 128), v(288, 128), v(288, 128), v(288, 128), v(48, 128)]
    dma = pltpu.SemaphoreType.DMA
    scratch += [dma((4,)), dma((COUNT, 2)), dma((COUNT, 2)), dma, dma]
    scratch += [pltpu.SemaphoreType.REGULAR] * 3
    vmem = pl.BlockSpec(memory_space=pltpu.VMEM)
    velocity, compressed = pl.pallas_call(
        functools.partial(kernel, sizes),
        out_shape=(
            jax.ShapeDtypeStruct((384, 128), F32),
            jax.ShapeDtypeStruct((3, 16, per, 4 * n_gx), F32),
        ),
        in_specs=[pl.BlockSpec(memory_space=pltpu.HBM)] * 4,
        out_specs=(vmem, vmem),
        scratch_shapes=scratch,
        compiler_params=pltpu.CompilerParams(
            collective_id=0, has_side_effects=True, vmem_limit_bytes=12 * 2**20
        ),
        name="vcycle",
    )(
        *(
            pltpu.with_memory_space_constraint(value, pltpu.HBM)
            for value in (
                velocity_prev.reshape(384, 128), forcing.reshape(384, 128), reaction.reshape(128, 128),
                jnp.asarray(haar_matrix(n_gx)),
            )
        )
    )
    velocity, compressed = pl.pallas_call(
        put_kernel,
        out_shape=tuple(jax.ShapeDtypeStruct(value.shape, F32) for value in (velocity, compressed)),
        in_specs=[vmem] * 2,
        out_specs=[pl.BlockSpec(memory_space=pltpu.HBM)] * 2,
        scratch_shapes=[dma((2,))],
        compiler_params=pltpu.CompilerParams(vmem_limit_bytes=12 * 2**20),
        name="put",
    )(velocity, compressed)
    return velocity.reshape(3, 8, 16, 128), compressed


def solution(mesh):
    placed = (P(None, "gx", "gy", "agg"), P(None, "gx", "gy", "agg"), P("gx", "gy", "agg"))
    sizes = tuple(mesh.shape[name] for name in ("agg", "gx", "gy"))
    return jax.shard_map(
        functools.partial(on_device, sizes),
        mesh=mesh,
        in_specs=placed,
        out_specs=(P(None, "gx", "gy", "agg"), P(None, "gy", ("agg", "gx"), None)),
        check_vma=False,
    )
```

```python
import functools

import jax
import jax.numpy as jnp
import numpy as np
from jax import lax
from jax.experimental import pallas as pl
from jax.experimental.pallas import tpu as pltpu
from jax.sharding import PartitionSpec as P

SWEEPS = 2
COARSE_SWEEPS = 4
LX = 5
damping = 0.8
keep = 1.0 - damping
root_half = 0.7071067811865476
MESH = pl.DeviceIdType.MESH
F32 = jnp.float32

X1, Z1, X2, Z2, X3, Z3, XF2, ZF2, XF3, ZF3, DZ, DX, DXZ, BZ, BX, BXZ, Y1, Y2, Y3, Y4, COUNT = range(21)
ROW = 4
TURNS = (1, 1, 2, 2, 3, 3, 4, 5)

def haar_matrix(devices):
    size = 4 * devices
    approx = np.eye(size)
    details = []
    for _ in range(LX - 1):
        even, odd = approx[:, 0::2], approx[:, 1::2]
        approx, detail = (even + odd) * root_half, (even - odd) * root_half
        details.append(detail)
    whole = np.concatenate([approx] + details[::-1], axis=1)
    parts = whole.reshape(devices, 4, size)
    return np.concatenate([parts[:, m] for m in range(4)], axis=1).astype(np.float32)


def dot(a, b, dims=((1,), (0,))):
    return lax.dot_general(
        a, b, (dims, ((), ())), precision=lax.Precision.HIGHEST, preferred_element_type=F32
    )


def lanes(shape):
    return lax.broadcasted_iota(jnp.int32, shape, len(shape) - 1)


def rows(shape):
    return lax.broadcasted_iota(jnp.int32, shape, len(shape) - 2)


def kernel(
    sizes, vp_in, f_in, r_in, m_in, vel, comp,
    vp, f, r, mcat, c_ref, u1, u2, tp, sendt, recvt,
    xs, xr1, xr2, xr3, zs1, zr1, zs2, zr2, zs3, zr3,
    p1, p2, po, ps, xf2s, xf2r, zf2s, zf2r, xf3s, xf3r, zf3s, zf3r,
    y1s, y1r, y2s, y2r, y3s, y3r, y4s, y4r,
    down, dtile, dpack, dxr, dzs, dzr, dxz, bown, btile, bpack, bxr, bzs, bzr, bxz,
    cdext, cf, cz, eu, ph,
    insem, ssem, rsem, assem, arsem, ready, token_up, token_down,
):
    n_agg, n_gx, n_gy = sizes
    per = 128 // n_gx
    levels = n_gx // ROW
    axes = {"agg": n_agg, "gx": n_gx, "gy": n_gy}
    here = {name: lax.axis_index(name) for name in axes}
    gx = here["gx"]
    level, place_x = gx // ROW, lax.rem(gx, ROW)

    def upper(axis):
        return here[axis] < axes[axis] - 1

    def lower(axis):
        return here[axis] > 0

    for ref in (
        xr1, xr2, xr3, zr1, zr2, zr3, xf2r, zf2r, xf3r, zf3r, y1r, y2r, y3r, y4r, dzr, dxr, dxz, bzr, bxr, bxz
    ):
        ref[...] = jnp.zeros(ref.shape, F32)

    barrier = pltpu.get_barrier_semaphore()

    def greet(test, device):
        @pl.when(test)
        def _():
            pl.semaphore_signal(barrier, inc=1, device_id=device, device_id_type=MESH)

    crossing_up = jnp.logical_and(place_x == ROW - 1, upper("gx"))
    crossing_down = jnp.logical_and(place_x == 0, lower("gx"))
    last_pair = n_gy - 2
    gy = here["gy"]
    sure = ((gy == last_pair), jnp.logical_and(gy > 0, gy <= last_pair))
    later = ((gy < last_pair), (gy > last_pair))
    greet(gy < last_pair, {"gy": gy + 1})
    greet(gy > last_pair, {"gy": gy - 1})
    greet(upper("agg"), {"agg": here["agg"] + 1})
    greet(lower("agg"), {"agg": here["agg"] - 1})
    for step in range(1, ROW):
        pl.semaphore_signal(
            barrier, inc=1, device_id={"gx": level * ROW + lax.rem(place_x + step, ROW)}, device_id_type=MESH
        )
    greet(crossing_up, {"gx": gx + 1})
    greet(crossing_down, {"gx": gx - 1})
    greet(level < levels - 1, {"gx": gx + ROW})
    greet(level > 0, {"gx": gx - ROW})

    fetches = [
        pltpu.make_async_copy(source, ref, insem.at[k])
        for k, (source, ref) in enumerate(((vp_in, vp), (r_in, r), (f_in, f), (m_in, mcat)))
    ]
    for fetch in fetches:
        fetch.start()

    def one_copy(message, axis, src, dst, side):
        step = 1 if side == 0 else -1
        return pltpu.make_async_remote_copy(
            src_ref=src[side], dst_ref=dst.at[side],
            send_sem=ssem.at[message, side], recv_sem=rsem.at[message, side],
            device_id={axis: here[axis] + step}, device_id_type=MESH,
        )

    ends = []

    def send_y(message, src, dst, tests):
        for side, test in enumerate(tests):

            @pl.when(test)
            def _(side=side):
                one_copy(message, "gy", both(src), dst, side).start()

    def start(message, axis, src, dst, sides=(0, 1)):
        for side in sides:

            @pl.when(upper(axis) if side == 0 else lower(axis))
            def _(side=side):
                one_copy(message, axis, src, dst, side).start()

            ends.append((message, axis, src, dst, side))

    def arrive(message, axis, src, dst):
        for side in (0, 1):

            @pl.when(lower(axis) if side == 0 else upper(axis))
            def _(side=side):
                one_copy(message, axis, src, dst, side).wait_recv()

    def both(ref):
        return (ref.at[0], ref.at[1])

    lane8, lane16, lane128 = lanes((8, 128)), lanes((16, 128)), lanes((128, 128))
    sub8 = rows((8, 128))
    y_at = lax.rem(rows((128, 128)), 16)

    def comp_of(ref, c):
        return ref[c * 128 : (c + 1) * 128, :]

    def plane(ref, c, j):
        return ref[pl.ds(c * 128 + j, 8, stride=16), :]

    def put_plane(ref, c, j, value):
        ref[pl.ds(c * 128 + j, 8, stride=16), :] = value

    def z_pack(tiles, column, lane):
        packed = jnp.zeros(lane.shape, F32)
        for place, tile in enumerate(tiles):
            packed = jnp.where(lane == place, pltpu.roll(tile, (place - column) % 128, 1), packed)
        return packed

    def z_tiles(ref):
        return [ref[t * 16 : (t + 1) * 16, :] for t in range(24)]

    def x_stage(ref, stage):
        for c in range(3):
            xs[stage, 0, c] = ref[c * 128 + 112 : c * 128 + 128, :]
            xs[stage, 1, c] = ref[c * 128 : c * 128 + 16, :]

    def z_stage(ref, staging):
        tiles = z_tiles(ref)
        staging[0] = z_pack(tiles, 127, lane16)
        staging[1] = z_pack(tiles, 0, lane16)

    def spread(packed, c, lane_at):
        return jnp.concatenate(
            [pltpu.roll(packed, (lane_at - (c * 8 + x)) % 128, 1) for x in range(8)], axis=0
        )

    def around(u, x_low, x_high, z_low, z_high):
        total = jnp.concatenate([x_low, u[:112]], axis=0) + jnp.concatenate([u[16:], x_high], axis=0)
        total = total + jnp.where(lane128 == 0, z_low, pltpu.roll(u, 1, 1))
        total = total + jnp.where(lane128 == 127, z_high, pltpu.roll(u, 127, 1))
        total = total + jnp.where(y_at == 0, 0.0, pltpu.roll(u, 1, 0))
        return total + jnp.where(y_at == 15, 0.0, pltpu.roll(u, 127, 0))

    def edges(k, x_got, z_low, z_high):
        value = jnp.where(sub8 == 0, x_got[0, k : k + 1, :], 0.0)
        value = value + jnp.where(sub8 == 7, x_got[1, k : k + 1, :], 0.0)
        value = value + jnp.where(lane8 == 0, pltpu.roll(z_low, (-k) % 128, 1), 0.0)
        return value + jnp.where(lane8 == 127, pltpu.roll(z_high, 127 - k, 1), 0.0)

    def beside(p, k, x_got, z_low, z_high):
        near = jnp.where(sub8 == 0, 0.0, pltpu.roll(p, 1, 0)) + jnp.where(sub8 == 7, 0.0, pltpu.roll(p, 7, 0))
        near = near + jnp.where(lane8 == 0, 0.0, pltpu.roll(p, 1, 1))
        near = near + jnp.where(lane8 == 127, 0.0, pltpu.roll(p, 127, 1))
        return near + edges(k, x_got, z_low, z_high)

    faces = ((0, (15, 14)), (1, (0, 1)))
    mine = ((0, (0, 1)), (1, (15, 14)))

    halves = jnp.where(lax.shift_right_logical(rows((128, 128)), 1) == lane128, 0.125, 0.0)

    def tile_of(ref, t):
        return ref[t * 8 : t * 8 + 8, :]

    def stage_rows(own, staging, at, n):
        for c in range(n):
            a, b, d, e = (tile_of(own, c * 4 + i) for i in range(4))
            up0, up1 = (jnp.where(sub8 < 4, pltpu.roll(v, 4, 0), w) for v, w in ((a, b), (d, e)))
            dn0, dn1 = (jnp.where(sub8 < 4, v, pltpu.roll(w, 4, 0)) for v, w in ((a, b), (d, e)))
            staging[0, at + c] = jnp.where(lane8 < 64, up0, pltpu.roll(up1, 64, 1))
            staging[1, at + c] = jnp.where(lane8 < 64, dn0, pltpu.roll(dn1, 64, 1))

    def unstage_rows(got, at, tile, n):
        for c in range(n):
            for i in range(4):
                low, high = got[0, at + c], got[1, at + c]
                if i >= 2:
                    low, high = pltpu.roll(low, 64, 1), pltpu.roll(high, 64, 1)
                if i % 2 == 0:
                    value = jnp.where(sub8 < 4, high, pltpu.roll(low, 4, 0))
                else:
                    value = jnp.where(sub8 < 4, pltpu.roll(high, 4, 0), low)
                tile[(c * 4 + i) * 8 : (c * 4 + i + 1) * 8, :] = value

    def join(own, tile, pack, staging, n):
        lane = lanes((n * 32, 128))
        pack[...] = jnp.where(lane < 64, own[...], pltpu.roll(tile[...], 64, 1))
        group = lane8 // 4
        sides = [jnp.zeros((8, 128), F32), jnp.zeros((8, 128), F32)]
        for t in range(8 * n):
            value = tile_of(own, t) if t < 4 * n else tile_of(tile, t - 4 * n)
            for side, column in ((0, 60), (1, 0)):
                sides[side] = jnp.where(group == t, pltpu.roll(value, (4 * t - column) % 128, 1), sides[side])
        staging[0], staging[1] = sides

    def assemble(pack, z_got, x_got, xz_got, c, n):
        tiles_ = []
        for place in range(12):
            t = c * 4 + place % 4
            if 4 <= place < 8:
                value, low, high = tile_of(pack, t), z_got[0], z_got[1]
            else:
                side = 0 if place < 4 else 1
                value, low, high = x_got[side, t * 8 : t * 8 + 8, :], xz_got[side, 0], xz_got[side, 1]
            for part, at in ((value, t), (pltpu.roll(value, 64, 1), 4 * n + t)):
                edge = jnp.where(
                    lane8 < 68, pltpu.roll(high, (64 - 4 * at) % 128, 1),
                    jnp.where(lane8 >= 124, pltpu.roll(low, (124 - 4 * at) % 128, 1), 0.0),
                )
                tiles_.append(jnp.where(lane8 < 64, part, edge))
        return jnp.concatenate(tiles_, axis=0)

    def take_turn(turn):
        for way, token in ((1, token_up), (-1, token_down)):
            for n in range(levels):
                if TURNS[n] == turn:

                    @pl.when(level == (n if way == 1 else levels - 1 - n))
                    def _(n=n, way=way, token=token):
                        if n > 0:
                            pl.semaphore_wait(token, 1)
                        if n < levels - 1:
                            pl.semaphore_signal(
                                token, inc=1, device_id={"gx": gx + way * ROW}, device_id_type=MESH
                            )

    fetches[0].wait()
    x_stage(vp, 0)
    greeted = ROW - 1
    for test in (
        sure[0], sure[1], upper("agg"), lower("agg"), crossing_up, crossing_down, level < levels - 1, level > 0
    ):
        greeted = greeted + test.astype(jnp.int32)
    pl.semaphore_wait(barrier, greeted)

    for test, step in zip(sure, (1, -1)):

        @pl.when(test)
        def _(step=step):
            pl.semaphore_signal(ready, inc=1, device_id={"gy": gy + step}, device_id_type=MESH)

    start(X1, "gx", both(xs.at[0]), xr1)
    z_stage(vp, zs1)
    start(Z1, "agg", both(zs1), zr1)

    fetches[1].wait()
    reaction = r[...]
    c_ref[...] = damping / (6.0 + reaction)
    halved = reaction.reshape(4, 2, 16, 128)
    tp[0:64, :] = (halved[:, 0] + halved[:, 1]).reshape(64, 128)
    mean_r = dot(tp[pl.ds(0, 32, stride=2), :] + tp[pl.ds(1, 32, stride=2), :], halves)
    inverse = damping / ((6.0 + 4.0 * mean_r) * 0.25)
    down[...] = inverse
    stage_rows(down, y1s, 5, 1)
    for slot, (j, k) in faces:
        for c in range(3):
            y1s[slot, c] = plane(vp, c, j)
        y1s[slot, 3] = c_ref[pl.ds(j, 8, stride=16), :]
        y1s[slot, 4] = c_ref[pl.ds(k, 8, stride=16), :]
    send_y(Y1, y1s, y1r, sure)
    fetches[2].wait()
    fetches[3].wait()

    first = []
    for c in range(3):
        pairs = comp_of(vp, c).reshape(4, 2, 16, 128)
        first.append(((pairs[:, 0] + pairs[:, 1]) * root_half).reshape(64, 128))
    a1 = jnp.concatenate(first, axis=0)
    even = lax.rem(rows((192, 128)), 2) == 0
    a1 = jnp.where(even, a1 + pltpu.roll(a1, 191, 0), pltpu.roll(a1, 1, 0) - a1) * root_half
    out_z, in_z = rows((128, 128)), lane128
    same = lax.shift_right_logical(out_z, 1) == lax.shift_right_logical(in_z, 1)
    minus = jnp.logical_and(lax.rem(out_z, 2) == 1, lax.rem(in_z, 2) == 1)
    pass_z = jnp.where(same, jnp.where(minus, -root_half, root_half), 0.0).astype(F32)
    turned = jnp.concatenate([dot(pass_z, a1, ((1,), (1,))), jnp.zeros((128, 64), F32)], axis=1)
    for t in range(n_gx):
        sendt[t] = turned[t * per : (t + 1) * per, :]

    arrive(X1, "gx", both(xs.at[0]), xr1)
    arrive(Z1, "agg", both(zs1), zr1)
    z_low, z_high = zr1[0], zr1[1]
    for c in range(3):
        u = comp_of(vp, c)
        total = comp_of(f, c) + around(
            u, xr1[0, c], xr1[1, c], spread(z_low, c, 0), spread(z_high, c, 127)
        )
        u1[c * 128 : (c + 1) * 128, :] = keep * u + c_ref[...] * total
    x_stage(u1, 1)
    start(X2, "gx", both(xs.at[1]), xr2)
    z_stage(u1, zs2)
    start(Z2, "agg", both(zs2), zr2)
    for slot, (j, _) in faces:
        for c in range(3):
            y2s[slot, c] = plane(u1, c, j)
    send_y(Y2, y2s, y2r, sure)
    take_turn(1)

    arrive(X2, "gx", both(xs.at[1]), xr2)
    arrive(Z2, "agg", both(zs2), zr2)
    z_low, z_high = zr2[0], zr2[1]
    for c in range(3):
        u = comp_of(u1, c)
        total = comp_of(f, c) + around(
            u, xr2[0, c], xr2[1, c], spread(z_low, c, 0), spread(z_high, c, 127)
        )
        u2[c * 128 : (c + 1) * 128, :] = keep * u + c_ref[...] * total
    x_stage(u2, 2)
    start(X3, "gx", both(xs.at[2]), xr3)
    z_stage(u2, zs3)
    start(Z3, "agg", both(zs3), zr3)
    for slot, (j, _) in faces:
        for c in range(3):
            y3s[slot, c] = plane(u2, c, j)
    send_y(Y3, y3s, y3r, sure)

    @pl.when(jnp.logical_or(later[0], later[1]))
    def _():
        pl.semaphore_wait(ready, 1)

    for message, src, dst in ((Y1, y1s, y1r), (Y2, y2s, y2r), (Y3, y3s, y3r)):
        send_y(message, src, dst, later)
        for side in (0, 1):
            ends.append((message, "gy", both(src), dst, side))
    take_turn(2)

    arrive(X3, "gx", both(xs.at[2]), xr3)
    arrive(Z3, "agg", both(zs3), zr3)
    z3_low, z3_high = zr3[0], zr3[1]
    for c in range(3):
        u = comp_of(u2, c)
        res = (
            comp_of(f, c) - (6.0 + r[...]) * u
            + around(u, xr3[0, c], xr3[1, c], spread(z3_low, c, 0), spread(z3_high, c, 127))
        )
        halved = res.reshape(4, 2, 16, 128)
        tp[c * 64 : (c + 1) * 64, :] = (
            (halved[:, 0] + halved[:, 1]).reshape(64, 128)
        )
    bown[...] = dot(tp[pl.ds(0, 96, stride=2), :] + tp[pl.ds(1, 96, stride=2), :], halves)
    stage_rows(bown, y4s, 0, 3)
    start(Y4, "gy", both(y4s), y4r)
    take_turn(3)


    arrive(Y1, "gy", both(y1s), y1r)
    unstage_rows(y1r, 5, dtile, 1)
    join(down, dtile, dpack, dzs, 1)
    start(DZ, "agg", both(dzs), dzr)
    start(DX, "gx", (dpack, dpack), dxr)
    take_turn(4)

    for side, (j, _) in mine:
        for c in range(3):
            k = side * 3 + c
            p1[k * 8 : k * 8 + 8, :] = c_ref[pl.ds(j, 8, stride=16), :] * y1r[side, c]
            p1[48 + k * 8 : 56 + k * 8, :] = y1r[side, 3] * plane(vp, c, j)
    xf2s[0, 0:12, :] = p1[pl.ds(7, 12, stride=8), :]
    xf2s[1, 0:12, :] = p1[pl.ds(0, 12, stride=8), :]
    start(XF2, "gx", both(xf2s), xf2r)
    tiles = [p1[k * 8 : k * 8 + 8, :] for k in range(12)]
    zf2s[0] = z_pack(tiles, 127, lane8)
    zf2s[1] = z_pack(tiles, 0, lane8)
    start(ZF2, "agg", both(zf2s), zf2r)

    take_turn(5)

    def send_line(step, carry):
        target = lax.rem(gx + step, n_gx)
        pltpu.make_async_remote_copy(
            src_ref=sendt.at[target], dst_ref=recvt.at[gx],
            send_sem=assem, recv_sem=arsem, device_id={"gx": target}, device_id_type=MESH,
        ).start()
        return carry

    lax.fori_loop(1, n_gx, send_line, 0)

    arrive(XF2, "gx", both(xf2s), xf2r)
    arrive(ZF2, "agg", both(zf2s), zf2r)
    arrive(Y2, "gy", both(y2s), y2r)
    f2_low, f2_high = zf2r[0], zf2r[1]
    for side, (j, j1) in mine:
        c0, c1 = c_ref[pl.ds(j, 8, stride=16), :], c_ref[pl.ds(j1, 8, stride=16), :]
        ch0, ch1 = y1r[side, 3], y1r[side, 4]
        for c in range(3):
            k = side * 3 + c
            own, halo = p1[k * 8 : k * 8 + 8, :], p1[48 + k * 8 : 56 + k * 8, :]
            near = beside(own, k, xf2r, f2_low, f2_high) + y2r[side, c] + halo
            p2[k * 8 : k * 8 + 8, :] = keep * own + c0 * near
            p2[48 + k * 8 : 56 + k * 8, :] = c1 * own
            near = beside(halo, 6 + k, xf2r, f2_low, f2_high) + plane(u1, c, j) + own
            p2[96 + k * 8 : 104 + k * 8, :] = keep * halo + ch0 * near
            p2[144 + k * 8 : 152 + k * 8, :] = ch1 * halo
            po[k * 8 : k * 8 + 8, :] = damping * (keep * plane(vp, c, j) + near)
    xf3s[0] = p2[pl.ds(7, 24, stride=8), :]
    xf3s[1] = p2[pl.ds(0, 24, stride=8), :]
    start(XF3, "gx", both(xf3s), xf3r)
    tiles = [p2[k * 8 : k * 8 + 8, :] for k in range(24)]
    zf3s[0] = z_pack(tiles, 127, lane8)
    zf3s[1] = z_pack(tiles, 0, lane8)
    start(ZF3, "agg", both(zf3s), zf3r)

    arrive(DZ, "agg", both(dzs), dzr)
    start(DXZ, "gx", (dzr, dzr), dxz)

    arrive(Y3, "gy", both(y3s), y3r)
    arrive(Y4, "gy", both(y4s), y4r)
    unstage_rows(y4r, 0, btile, 3)
    arrive(XF3, "gx", both(xf3s), xf3r)
    arrive(ZF3, "agg", both(zf3s), zf3r)
    f3_low, f3_high = zf3r[0], zf3r[1]
    for side, (j, j1) in mine:
        d0 = 6.0 + r[pl.ds(j, 8, stride=16), :]
        for c in range(3):
            k = side * 3 + c
            own0, own1, halo0, halo1 = (p2[n * 48 + k * 8 : n * 48 + k * 8 + 8, :] for n in range(4))
            whole0 = plane(u2, c, j) + own0
            beyond0 = y3r[side, c] + halo0
            near = beside(own0, k, xf3r, f3_low, f3_high) + beside(own1, 6 + k, xf3r, f3_low, f3_high)
            ps[k * 8 : k * 8 + 8, :] = (
                near + own1 + beyond0 + own0 - d0 * own0 - damping * p1[k * 8 : k * 8 + 8, :]
            )
            ps[48 + k * 8 : 56 + k * 8, :] = own1
            near = beside(halo0, 12 + k, xf3r, f3_low, f3_high) + beside(halo1, 18 + k, xf3r, f3_low, f3_high)
            ps[96 + k * 8 : 104 + k * 8, :] = (
                near + halo1 + whole0 + halo0 - po[k * 8 : k * 8 + 8, :] - damping * p1[48 + k * 8 : 56 + k * 8, :]
            )
            ps[144 + k * 8 : 152 + k * 8, :] = halo1
            put_plane(u2, c, j, whole0)
            put_plane(u2, c, j1, plane(u2, c, j1) + own1)
            ph[k * 8 : k * 8 + 8, :] = beyond0
    line = dot(ps[pl.ds(0, 96, stride=2), :] + ps[pl.ds(1, 96, stride=2), :], halves)
    for side in (0, 1):
        at0, at1 = ((0, 1), (7, 6))[side]
        to0, to1 = ((7, 6), (0, 1))[side]
        for c in range(3):
            k = (side * 3 + c) * 4
            for ref, row0, row1, base in ((bown, at0, at1, 0), (btile, to0, to1, 48)):
                for row, part in ((row0, k), (row1, 24 + k)):
                    at = pl.ds(c * 32 + row, 4, stride=8)
                    ref[at, :] = ref[at, :] + line[base + part : base + part + 4]
    join(bown, btile, bpack, bzs, 3)
    start(BZ, "agg", both(bzs), bzr)
    start(BX, "gx", (bpack, bpack), bxr)

    arrive(DX, "gx", (dpack, dpack), dxr)
    arrive(DXZ, "gx", (dzr, dzr), dxz)
    cdext[...] = assemble(dpack, dzr, dxr, dxz, 0, 1)

    arrive(BZ, "agg", both(bzs), bzr)
    start(BXZ, "gx", (bzr, bzr), bxz)

    many = n_gx - 1
    lines = pltpu.make_async_remote_copy(
        src_ref=sendt.at[pl.ds(0, many)], dst_ref=recvt.at[pl.ds(0, many)],
        send_sem=assem, recv_sem=arsem, device_id={"gx": lax.rem(gx + 1, n_gx)}, device_id_type=MESH,
    )
    lines.wait_recv()
    lines.wait_send()
    recvt[gx] = sendt[gx]
    for k in range(per):
        got = recvt[:, k, :]
        wide = dot(got[:, 0:192], mcat[...], ((0,), (0,)))
        for c in range(3):
            value = 0.0
            for m in range(4):
                at = (c * 4 + m) * 16
                value = value + wide[at : at + 16, m * 4 * n_gx : (m + 1) * 4 * n_gx]
            comp[c, :, k, :] = value

    arrive(BX, "gx", (bpack, bpack), bxr)
    arrive(BXZ, "gx", (bzr, bzr), bxz)

    y16 = lax.rem(rows((192, 128)), 16)
    fine = lane128 // 2 == rows((128, 128))
    beyond = jnp.logical_or(
        jnp.logical_and(lane128 == 0, rows((128, 128)) == 127),
        jnp.logical_and(lane128 == 127, rows((128, 128)) == 64),
    )
    up = jnp.concatenate([jnp.where(fine, 1.0, 0.0), jnp.where(beyond, 1.0, 0.0)], axis=1).astype(F32)
    none = jnp.zeros((16, 128), F32)
    for c in range(3):
        rhs_c = assemble(bpack, bzr, bxr, bxz, c, 3)
        weight = cdext[...]
        e = weight * rhs_c
        for _ in range(COARSE_SWEEPS - 1):
            near = jnp.concatenate([none, e[:176]], axis=0) + jnp.concatenate([e[16:], none], axis=0)
            near = near + pltpu.roll(e, 1, 1) + pltpu.roll(e, 127, 1)
            near = near + jnp.where(y16 == 0, pltpu.roll(e, 192 - 15, 0), pltpu.roll(e, 1, 0))
            near = near + jnp.where(y16 == 15, pltpu.roll(e, 15, 0), pltpu.roll(e, 191, 0))
            e = keep * e + weight * (rhs_c + 0.25 * near)
        refined = dot(e[48:144], up)
        eu[c * 96 : (c + 1) * 96, :] = refined[:, 0:128]
        for ref, part in ((cf, refined[:, 0:128]), (cz, refined[:, 128:256])):
            main = part.reshape(6, 16, 128)[:, 0:8].reshape(48, 128)
            ref[pl.ds(c * 96, 48, stride=2), :] = main
            ref[pl.ds(c * 96 + 1, 48, stride=2), :] = main
        for side, row in ((0, 15), (1, 8)):
            line_ = eu[pl.ds(c * 96 + 16 + row, 4, stride=16), :]
            at = (side * 3 + c) * 8
            for step in (0, 1):
                spot = pl.ds(at + step, 4, stride=2)
                ph[spot, :] = ph[spot, :] + line_

    def doubled(ref, c):
        value = ref[c * 96 + 16 : c * 96 + 80, :].reshape(4, 1, 16, 128)
        return jnp.broadcast_to(value, (4, 2, 16, 128)).reshape(128, 128)

    for c in range(3):
        w = comp_of(u2, c) + doubled(cf, c)
        outer = doubled(cz, c)
        total = comp_of(f, c) + around(
            w,
            xr3[0, c] + cf[c * 96 : c * 96 + 16, :],
            xr3[1, c] + cf[c * 96 + 80 : c * 96 + 96, :],
            spread(z3_low, c, 0) + outer,
            spread(z3_high, c, 127) + outer,
        )
        vel[c * 128 : (c + 1) * 128, :] = keep * w + c_ref[...] * total
    for side, (j, j1) in mine:
        c0, c1 = c_ref[pl.ds(j, 8, stride=16), :], c_ref[pl.ds(j1, 8, stride=16), :]
        for c in range(3):
            k = side * 3 + c
            more = edges(k, xf3r, f3_low, f3_high)
            more = more + ph[k * 8 : k * 8 + 8, :]
            put_plane(vel, c, j, plane(vel, c, j) + c0 * more)
            more = edges(6 + k, xf3r, f3_low, f3_high)
            put_plane(vel, c, j1, plane(vel, c, j1) + c1 * more)

    for message, axis, src, dst, side in ends:

        @pl.when(upper(axis) if side == 0 else lower(axis))
        def _(args=(message, axis, src, dst, side)):
            one_copy(*args).wait_send()


def put_kernel(velocity, compressed, velocity_out, compressed_out, sem):
    copies = [
        pltpu.make_async_copy(velocity, velocity_out, sem.at[0]),
        pltpu.make_async_copy(compressed, compressed_out, sem.at[1]),
    ]
    for copy in copies:
        copy.start()
    for copy in copies:
        copy.wait()


def on_device(sizes, velocity_prev, forcing, reaction):
    n_agg, n_gx, n_gy = sizes
    per = 128 // n_gx

    def v(*shape):
        return pltpu.VMEM(shape, F32)

    scratch = [
        v(384, 128), v(384, 128), v(128, 128), v(n_gx, 16 * n_gx),
        v(128, 128), v(384, 128), v(384, 128), v(192, 128),
        v(n_gx, per, 256), v(n_gx, per, 256),
        v(3, 2, 3, 16, 128), v(2, 3, 16, 128), v(2, 3, 16, 128), v(2, 3, 16, 128),
    ]
    scratch += [v(2, 16, 128)] * 6
    scratch += [v(96, 128), v(192, 128), v(48, 128), v(192, 128)]
    scratch += [v(2, 16, 128)] * 2 + [v(2, 8, 128)] * 2 + [v(2, 24, 128)] * 2 + [v(2, 8, 128)] * 2
    scratch += [v(2, 6, 8, 128)] * 2 + [v(2, 3, 8, 128)] * 6
    for n in (1, 3):
        scratch += [v(n * 32, 128)] * 3 + [v(2, n * 32, 128), v(2, 8, 128), v(2, 8, 128), v(2, 2, 8, 128)]
    scratch += [v(192, 128), v(288, 128), v(288, 128), v(288, 128), v(48, 128)]
    dma = pltpu.SemaphoreType.DMA
    scratch += [dma((4,)), dma((COUNT, 2)), dma((COUNT, 2)), dma, dma]
    scratch += [pltpu.SemaphoreType.REGULAR] * 3
    vmem = pl.BlockSpec(memory_space=pltpu.VMEM)
    velocity, compressed = pl.pallas_call(
        functools.partial(kernel, sizes),
        out_shape=(
            jax.ShapeDtypeStruct((384, 128), F32),
            jax.ShapeDtypeStruct((3, 16, per, 4 * n_gx), F32),
        ),
        in_specs=[pl.BlockSpec(memory_space=pltpu.HBM)] * 4,
        out_specs=(vmem, vmem),
        scratch_shapes=scratch,
        compiler_params=pltpu.CompilerParams(
            collective_id=0, has_side_effects=True, vmem_limit_bytes=12 * 2**20
        ),
        name="vcycle",
    )(
        *(
            pltpu.with_memory_space_constraint(value, pltpu.HBM)
            for value in (
                velocity_prev.reshape(384, 128), forcing.reshape(384, 128), reaction.reshape(128, 128),
                jnp.asarray(haar_matrix(n_gx)),
            )
        )
    )
    velocity, compressed = pl.pallas_call(
        put_kernel,
        out_shape=tuple(jax.ShapeDtypeStruct(value.shape, F32) for value in (velocity, compressed)),
        in_specs=[vmem] * 2,
        out_specs=[pl.BlockSpec(memory_space=pltpu.HBM)] * 2,
        scratch_shapes=[dma((2,))],
        compiler_params=pltpu.CompilerParams(vmem_limit_bytes=12 * 2**20),
        name="put",
    )(velocity, compressed)
    return velocity.reshape(3, 8, 16, 128), compressed


def solution(mesh):
    placed = (P(None, "gx", "gy", "agg"), P(None, "gx", "gy", "agg"), P("gx", "gy", "agg"))
    sizes = tuple(mesh.shape[name] for name in ("agg", "gx", "gy"))
    return jax.shard_map(
        functools.partial(on_device, sizes),
        mesh=mesh,
        in_specs=placed,
        out_specs=(P(None, "gx", "gy", "agg"), P(None, "gy", ("agg", "gx"), None)),
        check_vma=False,
    )
```

```python
import functools

import jax
import jax.numpy as jnp
import numpy as np
from jax import lax
from jax.experimental import pallas as pl
from jax.experimental.pallas import tpu as pltpu
from jax.sharding import PartitionSpec as P

SWEEPS = 2
COARSE_SWEEPS = 4
LX = 5
damping = 0.8
keep = 1.0 - damping
root_half = 0.7071067811865476
MESH = pl.DeviceIdType.MESH
F32 = jnp.float32

X1, Z1, X2, Z2, X3, Z3, XF2, ZF2, XF3, ZF3, DZ, DX, DXZ, BZ, BX, BXZ, Y1, Y2, Y3, Y4, XC, COUNT = range(22)
ROW = 4
TURNS = (1, 1, 2, 2, 3, 3, 4, 5)

def haar_matrix(devices):
    size = 4 * devices
    approx = np.eye(size)
    details = []
    for _ in range(LX - 1):
        even, odd = approx[:, 0::2], approx[:, 1::2]
        approx, detail = (even + odd) * root_half, (even - odd) * root_half
        details.append(detail)
    whole = np.concatenate([approx] + details[::-1], axis=1)
    parts = whole.reshape(devices, 4, size)
    return np.concatenate([parts[:, m] for m in range(4)], axis=1).astype(np.float32)


def dot(a, b, dims=((1,), (0,))):
    return lax.dot_general(
        a, b, (dims, ((), ())), precision=lax.Precision.HIGHEST, preferred_element_type=F32
    )


def lanes(shape):
    return lax.broadcasted_iota(jnp.int32, shape, len(shape) - 1)


def rows(shape):
    return lax.broadcasted_iota(jnp.int32, shape, len(shape) - 2)


def kernel(
    sizes, vp_in, f_in, r_in, m_in, vel, comp,
    vp, f, r, mcat, c_ref, u1, u2, tp, sendt, recvt,
    xs, xr1, xr2, xr3, xcs, xcr, zs1, zr1, zs2, zr2, zs3, zr3,
    p1, p2, po, ps, xf2s, xf2r, zf2s, zf2r, xf3s, xf3r, zf3s, zf3r,
    y1s, y1r, y2s, y2r, y3s, y3r, y4s, y4r,
    down, dtile, dpack, dxr, dzs, dzr, dxz, bown, btile, bpack, bxr, bzs, bzr, bxz,
    cdext, cf, cz, eu, ph,
    insem, ssem, rsem, assem, arsem, ready, token_up, token_down,
):
    n_agg, n_gx, n_gy = sizes
    per = 128 // n_gx
    levels = n_gx // ROW
    axes = {"agg": n_agg, "gx": n_gx, "gy": n_gy}
    here = {name: lax.axis_index(name) for name in axes}
    gx = here["gx"]
    level, place_x = gx // ROW, lax.rem(gx, ROW)

    def upper(axis):
        return here[axis] < axes[axis] - 1

    def lower(axis):
        return here[axis] > 0

    for ref in (
        xr1, xr2, xr3, xcr, zr1, zr2, zr3, xf2r, zf2r, xf3r, zf3r, y1r, y2r, y3r, y4r, dzr, dxr, dxz, bzr, bxr, bxz
    ):
        ref[...] = jnp.zeros(ref.shape, F32)

    barrier = pltpu.get_barrier_semaphore()

    def greet(test, device):
        @pl.when(test)
        def _():
            pl.semaphore_signal(barrier, inc=1, device_id=device, device_id_type=MESH)

    crossing_up = jnp.logical_and(place_x == ROW - 1, upper("gx"))
    crossing_down = jnp.logical_and(place_x == 0, lower("gx"))
    last_pair = n_gy - 1
    gy = here["gy"]
    sure = (jnp.logical_and(gy == last_pair, upper("gy")), jnp.logical_and(gy > 0, gy <= last_pair))
    later = ((gy < last_pair), (gy > last_pair))
    greet(gy < last_pair, {"gy": gy + 1})
    greet(gy > last_pair, {"gy": gy - 1})
    greet(upper("agg"), {"agg": here["agg"] + 1})
    greet(lower("agg"), {"agg": here["agg"] - 1})
    for step in range(1, ROW):
        pl.semaphore_signal(
            barrier, inc=1, device_id={"gx": level * ROW + lax.rem(place_x + step, ROW)}, device_id_type=MESH
        )
    greet(crossing_up, {"gx": gx + 1})
    greet(crossing_down, {"gx": gx - 1})
    greet(level < levels - 1, {"gx": gx + ROW})
    greet(level > 0, {"gx": gx - ROW})

    fetches = [
        pltpu.make_async_copy(source, ref, insem.at[k])
        for k, (source, ref) in enumerate(((vp_in, vp), (r_in, r), (f_in, f), (m_in, mcat)))
    ]
    for fetch in fetches:
        fetch.start()

    def one_copy(message, axis, src, dst, side):
        step = 1 if side == 0 else -1
        return pltpu.make_async_remote_copy(
            src_ref=src[side], dst_ref=dst.at[side],
            send_sem=ssem.at[message, side], recv_sem=rsem.at[message, side],
            device_id={axis: here[axis] + step}, device_id_type=MESH,
        )

    ends = []

    def send_y(message, src, dst, tests):
        for side, test in enumerate(tests):

            @pl.when(test)
            def _(side=side):
                one_copy(message, "gy", both(src), dst, side).start()

    def start(message, axis, src, dst, sides=(0, 1)):
        for side in sides:

            @pl.when(upper(axis) if side == 0 else lower(axis))
            def _(side=side):
                one_copy(message, axis, src, dst, side).start()

            ends.append((message, axis, src, dst, side))

    def arrive(message, axis, src, dst):
        for side in (0, 1):

            @pl.when(lower(axis) if side == 0 else upper(axis))
            def _(side=side):
                one_copy(message, axis, src, dst, side).wait_recv()

    def both(ref):
        return (ref.at[0], ref.at[1])

    lane8, lane16, lane128 = lanes((8, 128)), lanes((16, 128)), lanes((128, 128))
    sub8 = rows((8, 128))
    y_at = lax.rem(rows((128, 128)), 16)

    def comp_of(ref, c):
        return ref[c * 128 : (c + 1) * 128, :]

    def plane(ref, c, j):
        return ref[pl.ds(c * 128 + j, 8, stride=16), :]

    def put_plane(ref, c, j, value):
        ref[pl.ds(c * 128 + j, 8, stride=16), :] = value

    def z_pack(tiles, column, lane):
        packed = jnp.zeros(lane.shape, F32)
        for place, tile in enumerate(tiles):
            packed = jnp.where(lane == place, pltpu.roll(tile, (place - column) % 128, 1), packed)
        return packed

    def z_tiles(ref):
        return [ref[t * 16 : (t + 1) * 16, :] for t in range(24)]

    def x_stage(ref, stage):
        for c in range(3):
            xs[stage, 0, c] = ref[c * 128 + 112 : c * 128 + 128, :]
            xs[stage, 1, c] = ref[c * 128 : c * 128 + 16, :]

    def z_stage(ref, staging):
        tiles = z_tiles(ref)
        staging[0] = z_pack(tiles, 127, lane16)
        staging[1] = z_pack(tiles, 0, lane16)

    def spread(packed, c, lane_at):
        return jnp.concatenate(
            [pltpu.roll(packed, (lane_at - (c * 8 + x)) % 128, 1) for x in range(8)], axis=0
        )

    def around(u, x_low, x_high, z_low, z_high):
        total = jnp.concatenate([x_low, u[:112]], axis=0) + jnp.concatenate([u[16:], x_high], axis=0)
        total = total + jnp.where(lane128 == 0, z_low, pltpu.roll(u, 1, 1))
        total = total + jnp.where(lane128 == 127, z_high, pltpu.roll(u, 127, 1))
        total = total + jnp.where(y_at == 0, 0.0, pltpu.roll(u, 1, 0))
        return total + jnp.where(y_at == 15, 0.0, pltpu.roll(u, 127, 0))

    def edges(k, x_got, z_low, z_high):
        value = jnp.where(sub8 == 0, x_got[0, k : k + 1, :], 0.0)
        value = value + jnp.where(sub8 == 7, x_got[1, k : k + 1, :], 0.0)
        value = value + jnp.where(lane8 == 0, pltpu.roll(z_low, (-k) % 128, 1), 0.0)
        return value + jnp.where(lane8 == 127, pltpu.roll(z_high, 127 - k, 1), 0.0)

    def beside(p, k, x_got, z_low, z_high):
        near = jnp.where(sub8 == 0, 0.0, pltpu.roll(p, 1, 0)) + jnp.where(sub8 == 7, 0.0, pltpu.roll(p, 7, 0))
        near = near + jnp.where(lane8 == 0, 0.0, pltpu.roll(p, 1, 1))
        near = near + jnp.where(lane8 == 127, 0.0, pltpu.roll(p, 127, 1))
        return near + edges(k, x_got, z_low, z_high)

    faces = ((0, (15, 14)), (1, (0, 1)))
    mine = ((0, (0, 1)), (1, (15, 14)))

    halves = jnp.where(lax.shift_right_logical(rows((128, 128)), 1) == lane128, 0.125, 0.0)

    def tile_of(ref, t):
        return ref[t * 8 : t * 8 + 8, :]

    def stage_rows(own, staging, at, n):
        for c in range(n):
            a, b, d, e = (tile_of(own, c * 4 + i) for i in range(4))
            up0, up1 = (jnp.where(sub8 < 4, pltpu.roll(v, 4, 0), w) for v, w in ((a, b), (d, e)))
            dn0, dn1 = (jnp.where(sub8 < 4, v, pltpu.roll(w, 4, 0)) for v, w in ((a, b), (d, e)))
            staging[0, at + c] = jnp.where(lane8 < 64, up0, pltpu.roll(up1, 64, 1))
            staging[1, at + c] = jnp.where(lane8 < 64, dn0, pltpu.roll(dn1, 64, 1))

    def unstage_rows(got, at, tile, n):
        for c in range(n):
            for i in range(4):
                low, high = got[0, at + c], got[1, at + c]
                if i >= 2:
                    low, high = pltpu.roll(low, 64, 1), pltpu.roll(high, 64, 1)
                if i % 2 == 0:
                    value = jnp.where(sub8 < 4, high, pltpu.roll(low, 4, 0))
                else:
                    value = jnp.where(sub8 < 4, pltpu.roll(high, 4, 0), low)
                tile[(c * 4 + i) * 8 : (c * 4 + i + 1) * 8, :] = value

    def join(own, tile, pack, staging, n):
        lane = lanes((n * 32, 128))
        pack[...] = jnp.where(lane < 64, own[...], pltpu.roll(tile[...], 64, 1))
        group = lane8 // 4
        sides = [jnp.zeros((8, 128), F32), jnp.zeros((8, 128), F32)]
        for t in range(8 * n):
            value = tile_of(own, t) if t < 4 * n else tile_of(tile, t - 4 * n)
            for side, column in ((0, 60), (1, 0)):
                sides[side] = jnp.where(group == t, pltpu.roll(value, (4 * t - column) % 128, 1), sides[side])
        staging[0], staging[1] = sides

    def assemble(pack, z_got, x_got, xz_got, c, n):
        tiles_ = []
        for place in range(12):
            t = c * 4 + place % 4
            if 4 <= place < 8:
                value, low, high = tile_of(pack, t), z_got[0], z_got[1]
            else:
                side = 0 if place < 4 else 1
                value, low, high = x_got[side, t * 8 : t * 8 + 8, :], xz_got[side, 0], xz_got[side, 1]
            for part, at in ((value, t), (pltpu.roll(value, 64, 1), 4 * n + t)):
                edge = jnp.where(
                    lane8 < 68, pltpu.roll(high, (64 - 4 * at) % 128, 1),
                    jnp.where(lane8 >= 124, pltpu.roll(low, (124 - 4 * at) % 128, 1), 0.0),
                )
                tiles_.append(jnp.where(lane8 < 64, part, edge))
        return jnp.concatenate(tiles_, axis=0)

    def take_turn(turn):
        for way, token in ((1, token_up), (-1, token_down)):
            for n in range(levels):
                if TURNS[n] == turn:

                    @pl.when(level == (n if way == 1 else levels - 1 - n))
                    def _(n=n, way=way, token=token):
                        if n > 0:
                            pl.semaphore_wait(token, 1)
                        if n < levels - 1:
                            pl.semaphore_signal(
                                token, inc=1, device_id={"gx": gx + way * ROW}, device_id_type=MESH
                            )

    fetches[0].wait()
    x_stage(vp, 0)
    greeted = ROW - 1
    for test in (
        sure[0], sure[1], upper("agg"), lower("agg"), crossing_up, crossing_down, level < levels - 1, level > 0
    ):
        greeted = greeted + test.astype(jnp.int32)
    pl.semaphore_wait(barrier, greeted)

    for test, step in zip(sure, (1, -1)):

        @pl.when(test)
        def _(step=step):
            pl.semaphore_signal(ready, inc=1, device_id={"gy": gy + step}, device_id_type=MESH)

    start(X1, "gx", both(xs.at[0]), xr1)
    z_stage(vp, zs1)
    start(Z1, "agg", both(zs1), zr1)

    fetches[1].wait()
    reaction = r[...]
    c_ref[...] = damping / (6.0 + reaction)
    halved = reaction.reshape(4, 2, 16, 128)
    tp[0:64, :] = (halved[:, 0] + halved[:, 1]).reshape(64, 128)
    mean_r = dot(tp[pl.ds(0, 32, stride=2), :] + tp[pl.ds(1, 32, stride=2), :], halves)
    inverse = damping / ((6.0 + 4.0 * mean_r) * 0.25)
    down[...] = inverse
    stage_rows(down, y2s, 3, 1)
    for slot, (j, k) in faces:
        for c in range(3):
            y1s[slot, c] = plane(vp, c, j)
        y1s[slot, 3] = c_ref[pl.ds(j, 8, stride=16), :]
        y3s[slot, 3] = c_ref[pl.ds(k, 8, stride=16), :]
    send_y(Y1, y1s, y1r, sure)
    fetches[2].wait()
    fetches[3].wait()

    first = []
    for c in range(3):
        pairs = comp_of(vp, c).reshape(4, 2, 16, 128)
        first.append(((pairs[:, 0] + pairs[:, 1]) * root_half).reshape(64, 128))
    a1 = jnp.concatenate(first, axis=0)
    even = lax.rem(rows((192, 128)), 2) == 0
    a1 = jnp.where(even, a1 + pltpu.roll(a1, 191, 0), pltpu.roll(a1, 1, 0) - a1) * root_half
    out_z, in_z = rows((128, 128)), lane128
    same = lax.shift_right_logical(out_z, 1) == lax.shift_right_logical(in_z, 1)
    minus = jnp.logical_and(lax.rem(out_z, 2) == 1, lax.rem(in_z, 2) == 1)
    pass_z = jnp.where(same, jnp.where(minus, -root_half, root_half), 0.0).astype(F32)
    turned = jnp.concatenate([dot(pass_z, a1, ((1,), (1,))), jnp.zeros((128, 64), F32)], axis=1)
    for t in range(n_gx):
        sendt[t] = turned[t * per : (t + 1) * per, :]

    arrive(X1, "gx", both(xs.at[0]), xr1)
    arrive(Z1, "agg", both(zs1), zr1)
    z_low, z_high = zr1[0], zr1[1]
    for c in range(3):
        u = comp_of(vp, c)
        total = comp_of(f, c) + around(
            u, xr1[0, c], xr1[1, c], spread(z_low, c, 0), spread(z_high, c, 127)
        )
        u1[c * 128 : (c + 1) * 128, :] = keep * u + c_ref[...] * total
    x_stage(u1, 1)
    start(X2, "gx", both(xs.at[1]), xr2)
    z_stage(u1, zs2)
    start(Z2, "agg", both(zs2), zr2)
    for slot, (j, _) in faces:
        for c in range(3):
            y2s[slot, c] = plane(u1, c, j)
    send_y(Y2, y2s, y2r, sure)
    take_turn(1)

    arrive(X2, "gx", both(xs.at[1]), xr2)
    arrive(Z2, "agg", both(zs2), zr2)
    z_low, z_high = zr2[0], zr2[1]
    for c in range(3):
        u = comp_of(u1, c)
        total = comp_of(f, c) + around(
            u, xr2[0, c], xr2[1, c], spread(z_low, c, 0), spread(z_high, c, 127)
        )
        u2[c * 128 : (c + 1) * 128, :] = keep * u + c_ref[...] * total
    x_stage(u2, 2)
    even, odd = pl.ds(0, 8, stride=2), pl.ds(1, 8, stride=2)
    sums = [xs[2, side, c, even, :] + xs[2, side, c, odd, :] for side in (0, 1) for c in range(3)]
    sums = dot(jnp.concatenate(sums, axis=0), halves)
    for side in (0, 1):
        first, second, third = (sums[(side * 3 + c) * 8 : (side * 3 + c + 1) * 8] for c in range(3))
        xcs[side, 0] = jnp.where(lane8 < 64, first, pltpu.roll(second, 64, 1))
        xcs[side, 1] = third
    start(XC, "gx", both(xcs), xcr)
    z_stage(u2, zs3)
    start(Z3, "agg", both(zs3), zr3)
    for slot, (j, _) in faces:
        for c in range(3):
            y3s[slot, c] = plane(u2, c, j)
    send_y(Y3, y3s, y3r, sure)

    @pl.when(jnp.logical_or(later[0], later[1]))
    def _():
        pl.semaphore_wait(ready, 1)

    for message, src, dst in ((Y1, y1s, y1r), (Y2, y2s, y2r), (Y3, y3s, y3r)):
        send_y(message, src, dst, later)
        for side in (0, 1):
            ends.append((message, "gy", both(src), dst, side))
    take_turn(2)

    arrive(Z3, "agg", both(zs3), zr3)
    z3_low, z3_high = zr3[0], zr3[1]
    none = jnp.zeros((16, 128), F32)
    for c in range(3):
        u = comp_of(u2, c)
        res = (
            comp_of(f, c) - (6.0 + r[...]) * u
            + around(u, none, none, spread(z3_low, c, 0), spread(z3_high, c, 127))
        )
        halved = res.reshape(4, 2, 16, 128)
        tp[c * 64 : (c + 1) * 64, :] = (
            (halved[:, 0] + halved[:, 1]).reshape(64, 128)
        )
    bown[...] = dot(tp[pl.ds(0, 96, stride=2), :] + tp[pl.ds(1, 96, stride=2), :], halves)
    arrive(XC, "gx", both(xcs), xcr)
    for side, i in ((0, 0), (1, 3)):
        parts = (xcr[side, 0], pltpu.roll(xcr[side, 0], 64, 1), xcr[side, 1])
        for c in range(3):
            at = (c * 4 + i) * 8
            bown[at : at + 8, :] = bown[at : at + 8, :] + parts[c]
    stage_rows(bown, y4s, 0, 3)
    start(Y4, "gy", both(y4s), y4r)
    take_turn(3)


    arrive(Y1, "gy", both(y1s), y1r)
    take_turn(4)

    for side, (j, _) in mine:
        for c in range(3):
            k = side * 3 + c
            p1[k * 8 : k * 8 + 8, :] = c_ref[pl.ds(j, 8, stride=16), :] * y1r[side, c]
            p1[48 + k * 8 : 56 + k * 8, :] = y1r[side, 3] * plane(vp, c, j)
    xf2s[0, 0:12, :] = p1[pl.ds(7, 12, stride=8), :]
    xf2s[1, 0:12, :] = p1[pl.ds(0, 12, stride=8), :]
    start(XF2, "gx", both(xf2s), xf2r)
    tiles = [p1[k * 8 : k * 8 + 8, :] for k in range(12)]
    zf2s[0] = z_pack(tiles, 127, lane8)
    zf2s[1] = z_pack(tiles, 0, lane8)
    start(ZF2, "agg", both(zf2s), zf2r)

    take_turn(5)

    def send_line(step, carry):
        target = lax.rem(gx + step, n_gx)
        pltpu.make_async_remote_copy(
            src_ref=sendt.at[target], dst_ref=recvt.at[gx],
            send_sem=assem, recv_sem=arsem, device_id={"gx": target}, device_id_type=MESH,
        ).start()
        return carry

    lax.fori_loop(1, n_gx, send_line, 0)

    arrive(XF2, "gx", both(xf2s), xf2r)
    arrive(ZF2, "agg", both(zf2s), zf2r)
    arrive(Y2, "gy", both(y2s), y2r)
    arrive(Y3, "gy", both(y3s), y3r)
    f2_low, f2_high = zf2r[0], zf2r[1]
    for side, (j, j1) in mine:
        c0, c1 = c_ref[pl.ds(j, 8, stride=16), :], c_ref[pl.ds(j1, 8, stride=16), :]
        ch0, ch1 = y1r[side, 3], y3r[side, 3]
        for c in range(3):
            k = side * 3 + c
            own, halo = p1[k * 8 : k * 8 + 8, :], p1[48 + k * 8 : 56 + k * 8, :]
            near = beside(own, k, xf2r, f2_low, f2_high) + y2r[side, c] + halo
            p2[k * 8 : k * 8 + 8, :] = keep * own + c0 * near
            p2[48 + k * 8 : 56 + k * 8, :] = c1 * own
            near = beside(halo, 6 + k, xf2r, f2_low, f2_high) + plane(u1, c, j) + own
            p2[96 + k * 8 : 104 + k * 8, :] = keep * halo + ch0 * near
            p2[144 + k * 8 : 152 + k * 8, :] = ch1 * halo
            po[k * 8 : k * 8 + 8, :] = damping * (keep * plane(vp, c, j) + near)
    xf3s[0] = p2[pl.ds(7, 24, stride=8), :]
    xf3s[1] = p2[pl.ds(0, 24, stride=8), :]
    start(XF3, "gx", both(xf3s), xf3r)
    tiles = [p2[k * 8 : k * 8 + 8, :] for k in range(24)]
    zf3s[0] = z_pack(tiles, 127, lane8)
    zf3s[1] = z_pack(tiles, 0, lane8)
    start(ZF3, "agg", both(zf3s), zf3r)

    start(X3, "gx", both(xs.at[2]), xr3)

    unstage_rows(y2r, 3, dtile, 1)
    join(down, dtile, dpack, dzs, 1)
    start(DZ, "agg", both(dzs), dzr)
    start(DX, "gx", (dpack, dpack), dxr)

    arrive(Y4, "gy", both(y4s), y4r)
    arrive(DZ, "agg", both(dzs), dzr)
    start(DXZ, "gx", (dzr, dzr), dxz)
    unstage_rows(y4r, 0, btile, 3)
    arrive(XF3, "gx", both(xf3s), xf3r)
    arrive(ZF3, "agg", both(zf3s), zf3r)
    f3_low, f3_high = zf3r[0], zf3r[1]
    for side, (j, j1) in mine:
        d0 = 6.0 + r[pl.ds(j, 8, stride=16), :]
        for c in range(3):
            k = side * 3 + c
            own0, own1, halo0, halo1 = (p2[n * 48 + k * 8 : n * 48 + k * 8 + 8, :] for n in range(4))
            whole0 = plane(u2, c, j) + own0
            beyond0 = y3r[side, c] + halo0
            near = beside(own0, k, xf3r, f3_low, f3_high) + beside(own1, 6 + k, xf3r, f3_low, f3_high)
            ps[k * 8 : k * 8 + 8, :] = (
                near + own1 + beyond0 + own0 - d0 * own0 - damping * p1[k * 8 : k * 8 + 8, :]
            )
            ps[48 + k * 8 : 56 + k * 8, :] = own1
            near = beside(halo0, 12 + k, xf3r, f3_low, f3_high) + beside(halo1, 18 + k, xf3r, f3_low, f3_high)
            ps[96 + k * 8 : 104 + k * 8, :] = (
                near + halo1 + whole0 + halo0 - po[k * 8 : k * 8 + 8, :] - damping * p1[48 + k * 8 : 56 + k * 8, :]
            )
            ps[144 + k * 8 : 152 + k * 8, :] = halo1
            put_plane(u2, c, j, whole0)
            put_plane(u2, c, j1, plane(u2, c, j1) + own1)
            ph[k * 8 : k * 8 + 8, :] = beyond0
    line = dot(ps[pl.ds(0, 96, stride=2), :] + ps[pl.ds(1, 96, stride=2), :], halves)
    for side in (0, 1):
        at0, at1 = ((0, 1), (7, 6))[side]
        to0, to1 = ((7, 6), (0, 1))[side]
        for c in range(3):
            k = (side * 3 + c) * 4
            for ref, row0, row1, base in ((bown, at0, at1, 0), (btile, to0, to1, 48)):
                for row, part in ((row0, k), (row1, 24 + k)):
                    at = pl.ds(c * 32 + row, 4, stride=8)
                    ref[at, :] = ref[at, :] + line[base + part : base + part + 4]
    join(bown, btile, bpack, bzs, 3)
    start(BZ, "agg", both(bzs), bzr)
    start(BX, "gx", (bpack, bpack), bxr)

    arrive(BZ, "agg", both(bzs), bzr)
    start(BXZ, "gx", (bzr, bzr), bxz)
    arrive(DX, "gx", (dpack, dpack), dxr)
    arrive(DXZ, "gx", (dzr, dzr), dxz)
    cdext[...] = assemble(dpack, dzr, dxr, dxz, 0, 1)

    many = n_gx - 1
    lines = pltpu.make_async_remote_copy(
        src_ref=sendt.at[pl.ds(0, many)], dst_ref=recvt.at[pl.ds(0, many)],
        send_sem=assem, recv_sem=arsem, device_id={"gx": lax.rem(gx + 1, n_gx)}, device_id_type=MESH,
    )
    lines.wait_recv()
    lines.wait_send()
    recvt[gx] = sendt[gx]
    for k in range(per):
        got = recvt[:, k, :]
        wide = dot(got[:, 0:192], mcat[...], ((0,), (0,)))
        for c in range(3):
            value = 0.0
            for m in range(4):
                at = (c * 4 + m) * 16
                value = value + wide[at : at + 16, m * 4 * n_gx : (m + 1) * 4 * n_gx]
            comp[c, :, k, :] = value

    arrive(BX, "gx", (bpack, bpack), bxr)
    arrive(BXZ, "gx", (bzr, bzr), bxz)

    y16 = lax.rem(rows((192, 128)), 16)
    fine = lane128 // 2 == rows((128, 128))
    beyond = jnp.logical_or(
        jnp.logical_and(lane128 == 0, rows((128, 128)) == 127),
        jnp.logical_and(lane128 == 127, rows((128, 128)) == 64),
    )
    up = jnp.concatenate([jnp.where(fine, 1.0, 0.0), jnp.where(beyond, 1.0, 0.0)], axis=1).astype(F32)
    for c in range(3):
        rhs_c = assemble(bpack, bzr, bxr, bxz, c, 3)
        weight = cdext[...]
        e = weight * rhs_c
        for _ in range(COARSE_SWEEPS - 1):
            near = jnp.concatenate([none, e[:176]], axis=0) + jnp.concatenate([e[16:], none], axis=0)
            near = near + pltpu.roll(e, 1, 1) + pltpu.roll(e, 127, 1)
            near = near + jnp.where(y16 == 0, pltpu.roll(e, 192 - 15, 0), pltpu.roll(e, 1, 0))
            near = near + jnp.where(y16 == 15, pltpu.roll(e, 15, 0), pltpu.roll(e, 191, 0))
            e = keep * e + weight * (rhs_c + 0.25 * near)
        refined = dot(e[48:144], up)
        eu[c * 96 : (c + 1) * 96, :] = refined[:, 0:128]
        for ref, part in ((cf, refined[:, 0:128]), (cz, refined[:, 128:256])):
            main = part.reshape(6, 16, 128)[:, 0:8].reshape(48, 128)
            ref[pl.ds(c * 96, 48, stride=2), :] = main
            ref[pl.ds(c * 96 + 1, 48, stride=2), :] = main
        for side, row in ((0, 15), (1, 8)):
            line_ = eu[pl.ds(c * 96 + 16 + row, 4, stride=16), :]
            at = (side * 3 + c) * 8
            for step in (0, 1):
                spot = pl.ds(at + step, 4, stride=2)
                ph[spot, :] = ph[spot, :] + line_

    arrive(X3, "gx", both(xs.at[2]), xr3)

    def doubled(ref, c):
        value = ref[c * 96 + 16 : c * 96 + 80, :].reshape(4, 1, 16, 128)
        return jnp.broadcast_to(value, (4, 2, 16, 128)).reshape(128, 128)

    for c in range(3):
        w = comp_of(u2, c) + doubled(cf, c)
        outer = doubled(cz, c)
        total = comp_of(f, c) + around(
            w,
            xr3[0, c] + cf[c * 96 : c * 96 + 16, :],
            xr3[1, c] + cf[c * 96 + 80 : c * 96 + 96, :],
            spread(z3_low, c, 0) + outer,
            spread(z3_high, c, 127) + outer,
        )
        vel[c * 128 : (c + 1) * 128, :] = keep * w + c_ref[...] * total
    for side, (j, j1) in mine:
        c0, c1 = c_ref[pl.ds(j, 8, stride=16), :], c_ref[pl.ds(j1, 8, stride=16), :]
        for c in range(3):
            k = side * 3 + c
            more = edges(k, xf3r, f3_low, f3_high)
            more = more + ph[k * 8 : k * 8 + 8, :]
            put_plane(vel, c, j, plane(vel, c, j) + c0 * more)
            more = edges(6 + k, xf3r, f3_low, f3_high)
            put_plane(vel, c, j1, plane(vel, c, j1) + c1 * more)

    for message, axis, src, dst, side in ends:

        @pl.when(upper(axis) if side == 0 else lower(axis))
        def _(args=(message, axis, src, dst, side)):
            one_copy(*args).wait_send()


def put_kernel(velocity, compressed, velocity_out, compressed_out, sem):
    copies = [
        pltpu.make_async_copy(velocity, velocity_out, sem.at[0]),
        pltpu.make_async_copy(compressed, compressed_out, sem.at[1]),
    ]
    for copy in copies:
        copy.start()
    for copy in copies:
        copy.wait()


def on_device(sizes, velocity_prev, forcing, reaction):
    n_agg, n_gx, n_gy = sizes
    per = 128 // n_gx

    def v(*shape):
        return pltpu.VMEM(shape, F32)

    scratch = [
        v(384, 128), v(384, 128), v(128, 128), v(n_gx, 16 * n_gx),
        v(128, 128), v(384, 128), v(384, 128), v(192, 128),
        v(n_gx, per, 256), v(n_gx, per, 256),
        v(3, 2, 3, 16, 128), v(2, 3, 16, 128), v(2, 3, 16, 128), v(2, 3, 16, 128),
        v(2, 2, 8, 128), v(2, 2, 8, 128),
    ]
    scratch += [v(2, 16, 128)] * 6
    scratch += [v(96, 128), v(192, 128), v(48, 128), v(192, 128)]
    scratch += [v(2, 16, 128)] * 2 + [v(2, 8, 128)] * 2 + [v(2, 24, 128)] * 2 + [v(2, 8, 128)] * 2
    scratch += [v(2, 4, 8, 128)] * 6 + [v(2, 3, 8, 128)] * 2
    for n in (1, 3):
        scratch += [v(n * 32, 128)] * 3 + [v(2, n * 32, 128), v(2, 8, 128), v(2, 8, 128), v(2, 2, 8, 128)]
    scratch += [v(192, 128), v(288, 128), v(288, 128), v(288, 128), v(48, 128)]
    dma = pltpu.SemaphoreType.DMA
    scratch += [dma((4,)), dma((COUNT, 2)), dma((COUNT, 2)), dma, dma]
    scratch += [pltpu.SemaphoreType.REGULAR] * 3
    vmem = pl.BlockSpec(memory_space=pltpu.VMEM)
    velocity, compressed = pl.pallas_call(
        functools.partial(kernel, sizes),
        out_shape=(
            jax.ShapeDtypeStruct((384, 128), F32),
            jax.ShapeDtypeStruct((3, 16, per, 4 * n_gx), F32),
        ),
        in_specs=[pl.BlockSpec(memory_space=pltpu.HBM)] * 4,
        out_specs=(vmem, vmem),
        scratch_shapes=scratch,
        compiler_params=pltpu.CompilerParams(
            collective_id=0, has_side_effects=True, vmem_limit_bytes=12 * 2**20
        ),
        name="vcycle",
    )(
        *(
            pltpu.with_memory_space_constraint(value, pltpu.HBM)
            for value in (
                velocity_prev.reshape(384, 128), forcing.reshape(384, 128), reaction.reshape(128, 128),
                jnp.asarray(haar_matrix(n_gx)),
            )
        )
    )
    velocity, compressed = pl.pallas_call(
        put_kernel,
        out_shape=tuple(jax.ShapeDtypeStruct(value.shape, F32) for value in (velocity, compressed)),
        in_specs=[vmem] * 2,
        out_specs=[pl.BlockSpec(memory_space=pltpu.HBM)] * 2,
        scratch_shapes=[dma((2,))],
        compiler_params=pltpu.CompilerParams(vmem_limit_bytes=12 * 2**20),
        name="put",
    )(velocity, compressed)
    return velocity.reshape(3, 8, 16, 128), compressed


def solution(mesh):
    placed = (P(None, "gx", "gy", "agg"), P(None, "gx", "gy", "agg"), P("gx", "gy", "agg"))
    sizes = tuple(mesh.shape[name] for name in ("agg", "gx", "gy"))
    return jax.shard_map(
        functools.partial(on_device, sizes),
        mesh=mesh,
        in_specs=placed,
        out_specs=(P(None, "gx", "gy", "agg"), P(None, "gy", ("agg", "gx"), None)),
        check_vma=False,
    )
```

```python
import functools

import jax
import jax.numpy as jnp
import numpy as np
from jax import lax
from jax.experimental import pallas as pl
from jax.experimental.pallas import tpu as pltpu
from jax.sharding import PartitionSpec as P

SWEEPS = 2
COARSE_SWEEPS = 4
LX = 5
damping = 0.8
keep = 1.0 - damping
root_half = 0.7071067811865476
MESH = pl.DeviceIdType.MESH
F32 = jnp.float32

X1, Z1, X2, Z2, X3, Z3, XF2, ZF2, XF3, ZF3, DZ, DX, BZ, BX, Y1, Y2, Y3, Y4, XC, COUNT = range(20)
ROW = 4
TURNS = (1, 1, 2, 2, 3, 3, 4, 5)

def haar_matrix(devices):
    size = 4 * devices
    approx = np.eye(size)
    details = []
    for _ in range(LX - 1):
        even, odd = approx[:, 0::2], approx[:, 1::2]
        approx, detail = (even + odd) * root_half, (even - odd) * root_half
        details.append(detail)
    whole = np.concatenate([approx] + details[::-1], axis=1)
    parts = whole.reshape(devices, 4, size)
    return np.concatenate([parts[:, m] for m in range(4)], axis=1).astype(np.float32)


def dot(a, b, dims=((1,), (0,))):
    return lax.dot_general(
        a, b, (dims, ((), ())), precision=lax.Precision.HIGHEST, preferred_element_type=F32
    )


def lanes(shape):
    return lax.broadcasted_iota(jnp.int32, shape, len(shape) - 1)


def rows(shape):
    return lax.broadcasted_iota(jnp.int32, shape, len(shape) - 2)


def kernel(
    sizes, vp_in, f_in, r_in, m_in, vel, comp,
    vp, f, r, mcat, c_ref, u1, u2, tp, sendt, recvt,
    xs, xr1, xr2, xr3, xcs, xcr, zs1, zr1, zs2, zr2, zs3, zr3,
    p1, p2, po, ps, xf2s, xf2r, zf2s, zf2r, xf3s, xf3r, zf3s, zf3r,
    y1s, y1r, y2s, y2r, y3s, y3r, y4s, y4r,
    down, dtile, dpack, dxr, dzs, dzr, dxz, bown, btile, bpack, bxr, bzs, bzr, bxz,
    cdext, cf, cz, eu, ph,
    insem, ssem, rsem, cssem, crsem, assem, arsem, ready, token_up, token_down,
):
    n_agg, n_gx, n_gy = sizes
    per = 128 // n_gx
    levels = n_gx // ROW
    axes = {"agg": n_agg, "gx": n_gx, "gy": n_gy}
    here = {name: lax.axis_index(name) for name in axes}
    gx = here["gx"]
    level, place_x = gx // ROW, lax.rem(gx, ROW)

    def upper(axis):
        return here[axis] < axes[axis] - 1

    def lower(axis):
        return here[axis] > 0

    for ref in (
        xr1, xr2, xr3, xcr, zr1, zr2, zr3, xf2r, zf2r, xf3r, zf3r, y1r, y2r, y3r, y4r, dzr, dxr, dxz, bzr, bxr, bxz
    ):
        ref[...] = jnp.zeros(ref.shape, F32)

    barrier = pltpu.get_barrier_semaphore()

    def greet(test, device):
        @pl.when(test)
        def _():
            pl.semaphore_signal(barrier, inc=1, device_id=device, device_id_type=MESH)

    crossing_up = jnp.logical_and(place_x == ROW - 1, upper("gx"))
    crossing_down = jnp.logical_and(place_x == 0, lower("gx"))
    last_pair = n_gy - 1
    gy = here["gy"]
    sure = (jnp.logical_and(gy == last_pair, upper("gy")), jnp.logical_and(gy > 0, gy <= last_pair))
    later = ((gy < last_pair), (gy > last_pair))
    greet(gy < last_pair, {"gy": gy + 1})
    greet(gy > last_pair, {"gy": gy - 1})
    greet(upper("agg"), {"agg": here["agg"] + 1})
    greet(lower("agg"), {"agg": here["agg"] - 1})
    for step in range(1, ROW):
        pl.semaphore_signal(
            barrier, inc=1, device_id={"gx": level * ROW + lax.rem(place_x + step, ROW)}, device_id_type=MESH
        )
    greet(crossing_up, {"gx": gx + 1})
    greet(crossing_down, {"gx": gx - 1})
    corners = [
        (x_side, z_side, sx, sz)
        for x_side, sx in ((0, 1), (1, -1))
        for z_side, sz in ((0, 1), (1, -1))
    ]

    def corner_there(sx, sz):
        return jnp.logical_and(
            upper("gx") if sx == 1 else lower("gx"), upper("agg") if sz == 1 else lower("agg")
        )

    for _, _, sx, sz in corners:
        greet(corner_there(sx, sz), {"gx": gx + sx, "agg": here["agg"] + sz})
    greet(level < levels - 1, {"gx": gx + ROW})
    greet(level > 0, {"gx": gx - ROW})

    fetches = [
        pltpu.make_async_copy(source, ref, insem.at[k])
        for k, (source, ref) in enumerate(((vp_in, vp), (r_in, r), (f_in, f), (m_in, mcat)))
    ]
    for fetch in fetches:
        fetch.start()

    def one_copy(message, axis, src, dst, side):
        step = 1 if side == 0 else -1
        return pltpu.make_async_remote_copy(
            src_ref=src[side], dst_ref=dst.at[side],
            send_sem=ssem.at[message, side], recv_sem=rsem.at[message, side],
            device_id={axis: here[axis] + step}, device_id_type=MESH,
        )

    ends = []

    def send_y(message, src, dst, tests):
        for side, test in enumerate(tests):

            @pl.when(test)
            def _(side=side):
                one_copy(message, "gy", both(src), dst, side).start()

    def start(message, axis, src, dst, sides=(0, 1)):
        for side in sides:

            @pl.when(upper(axis) if side == 0 else lower(axis))
            def _(side=side):
                one_copy(message, axis, src, dst, side).start()

            ends.append((message, axis, src, dst, side))

    def arrive(message, axis, src, dst):
        for side in (0, 1):

            @pl.when(lower(axis) if side == 0 else upper(axis))
            def _(side=side):
                one_copy(message, axis, src, dst, side).wait_recv()

    def corner_copy(kind, x_side, z_side, sx, sz):
        src, dst = ((dzs, dxz), (bzs, bxz))[kind]
        k = x_side * 2 + z_side
        return pltpu.make_async_remote_copy(
            src_ref=src.at[z_side], dst_ref=dst.at[x_side, z_side],
            send_sem=cssem.at[kind, k], recv_sem=crsem.at[kind, k],
            device_id={"gx": gx + sx, "agg": here["agg"] + sz}, device_id_type=MESH,
        )

    def start_corners(kind):
        for corner in corners:

            @pl.when(corner_there(*corner[2:]))
            def _(corner=corner):
                corner_copy(kind, *corner).start()

    def arrive_corners(kind):
        for corner in corners:

            @pl.when(corner_there(-corner[2], -corner[3]))
            def _(corner=corner):
                corner_copy(kind, *corner).wait_recv()

    def both(ref):
        return (ref.at[0], ref.at[1])

    lane8, lane16, lane128 = lanes((8, 128)), lanes((16, 128)), lanes((128, 128))
    sub8 = rows((8, 128))
    y_at = lax.rem(rows((128, 128)), 16)

    def comp_of(ref, c):
        return ref[c * 128 : (c + 1) * 128, :]

    def plane(ref, c, j):
        return ref[pl.ds(c * 128 + j, 8, stride=16), :]

    def put_plane(ref, c, j, value):
        ref[pl.ds(c * 128 + j, 8, stride=16), :] = value

    def z_pack(tiles, column, lane):
        packed = jnp.zeros(lane.shape, F32)
        for place, tile in enumerate(tiles):
            packed = jnp.where(lane == place, pltpu.roll(tile, (place - column) % 128, 1), packed)
        return packed

    def z_tiles(ref):
        return [ref[t * 16 : (t + 1) * 16, :] for t in range(24)]

    def x_stage(ref, stage):
        for c in range(3):
            xs[stage, 0, c] = ref[c * 128 + 112 : c * 128 + 128, :]
            xs[stage, 1, c] = ref[c * 128 : c * 128 + 16, :]

    def z_stage(ref, staging):
        tiles = z_tiles(ref)
        staging[0] = z_pack(tiles, 127, lane16)
        staging[1] = z_pack(tiles, 0, lane16)

    def spread(packed, c, lane_at):
        return jnp.concatenate(
            [pltpu.roll(packed, (lane_at - (c * 8 + x)) % 128, 1) for x in range(8)], axis=0
        )

    def around(u, x_low, x_high, z_low, z_high):
        total = jnp.concatenate([x_low, u[:112]], axis=0) + jnp.concatenate([u[16:], x_high], axis=0)
        total = total + jnp.where(lane128 == 0, z_low, pltpu.roll(u, 1, 1))
        total = total + jnp.where(lane128 == 127, z_high, pltpu.roll(u, 127, 1))
        total = total + jnp.where(y_at == 0, 0.0, pltpu.roll(u, 1, 0))
        return total + jnp.where(y_at == 15, 0.0, pltpu.roll(u, 127, 0))

    def edges(k, x_got, z_low, z_high):
        value = jnp.where(sub8 == 0, x_got[0, k : k + 1, :], 0.0)
        value = value + jnp.where(sub8 == 7, x_got[1, k : k + 1, :], 0.0)
        value = value + jnp.where(lane8 == 0, pltpu.roll(z_low, (-k) % 128, 1), 0.0)
        return value + jnp.where(lane8 == 127, pltpu.roll(z_high, 127 - k, 1), 0.0)

    def beside(p, k, x_got, z_low, z_high):
        near = jnp.where(sub8 == 0, 0.0, pltpu.roll(p, 1, 0)) + jnp.where(sub8 == 7, 0.0, pltpu.roll(p, 7, 0))
        near = near + jnp.where(lane8 == 0, 0.0, pltpu.roll(p, 1, 1))
        near = near + jnp.where(lane8 == 127, 0.0, pltpu.roll(p, 127, 1))
        return near + edges(k, x_got, z_low, z_high)

    faces = ((0, (15, 14)), (1, (0, 1)))
    mine = ((0, (0, 1)), (1, (15, 14)))

    halves = jnp.where(lax.shift_right_logical(rows((128, 128)), 1) == lane128, 0.125, 0.0)

    def tile_of(ref, t):
        return ref[t * 8 : t * 8 + 8, :]

    def stage_rows(own, staging, at, n):
        for c in range(n):
            a, b, d, e = (tile_of(own, c * 4 + i) for i in range(4))
            up0, up1 = (jnp.where(sub8 < 4, pltpu.roll(v, 4, 0), w) for v, w in ((a, b), (d, e)))
            dn0, dn1 = (jnp.where(sub8 < 4, v, pltpu.roll(w, 4, 0)) for v, w in ((a, b), (d, e)))
            staging[0, at + c] = jnp.where(lane8 < 64, up0, pltpu.roll(up1, 64, 1))
            staging[1, at + c] = jnp.where(lane8 < 64, dn0, pltpu.roll(dn1, 64, 1))

    def unstage_rows(got, at, tile, n):
        for c in range(n):
            for i in range(4):
                low, high = got[0, at + c], got[1, at + c]
                if i >= 2:
                    low, high = pltpu.roll(low, 64, 1), pltpu.roll(high, 64, 1)
                if i % 2 == 0:
                    value = jnp.where(sub8 < 4, high, pltpu.roll(low, 4, 0))
                else:
                    value = jnp.where(sub8 < 4, pltpu.roll(high, 4, 0), low)
                tile[(c * 4 + i) * 8 : (c * 4 + i + 1) * 8, :] = value

    def join(own, tile, pack, staging, n):
        lane = lanes((n * 32, 128))
        pack[...] = jnp.where(lane < 64, own[...], pltpu.roll(tile[...], 64, 1))
        group = lane8 // 4
        sides = [jnp.zeros((8, 128), F32), jnp.zeros((8, 128), F32)]
        for t in range(8 * n):
            value = tile_of(own, t) if t < 4 * n else tile_of(tile, t - 4 * n)
            for side, column in ((0, 60), (1, 0)):
                sides[side] = jnp.where(group == t, pltpu.roll(value, (4 * t - column) % 128, 1), sides[side])
        staging[0], staging[1] = sides

    def assemble(pack, z_got, x_got, xz_got, c, n):
        tiles_ = []
        for place in range(12):
            t = c * 4 + place % 4
            if 4 <= place < 8:
                value, low, high = tile_of(pack, t), z_got[0], z_got[1]
            else:
                side = 0 if place < 4 else 1
                value, low, high = x_got[side, t * 8 : t * 8 + 8, :], xz_got[side, 0], xz_got[side, 1]
            for part, at in ((value, t), (pltpu.roll(value, 64, 1), 4 * n + t)):
                edge = jnp.where(
                    lane8 < 68, pltpu.roll(high, (64 - 4 * at) % 128, 1),
                    jnp.where(lane8 >= 124, pltpu.roll(low, (124 - 4 * at) % 128, 1), 0.0),
                )
                tiles_.append(jnp.where(lane8 < 64, part, edge))
        return jnp.concatenate(tiles_, axis=0)

    def take_turn(turn):
        for way, token in ((1, token_up), (-1, token_down)):
            for n in range(levels):
                if TURNS[n] == turn:

                    @pl.when(level == (n if way == 1 else levels - 1 - n))
                    def _(n=n, way=way, token=token):
                        if n > 0:
                            pl.semaphore_wait(token, 1)
                        if n < levels - 1:
                            pl.semaphore_signal(
                                token, inc=1, device_id={"gx": gx + way * ROW}, device_id_type=MESH
                            )

    fetches[0].wait()
    x_stage(vp, 0)
    greeted = ROW - 1
    for test in (
        sure[0], sure[1], upper("agg"), lower("agg"), crossing_up, crossing_down, level < levels - 1, level > 0
    ):
        greeted = greeted + test.astype(jnp.int32)
    for _, _, sx, sz in corners:
        greeted = greeted + corner_there(sx, sz).astype(jnp.int32)
    pl.semaphore_wait(barrier, greeted)

    for test, step in zip(sure, (1, -1)):

        @pl.when(test)
        def _(step=step):
            pl.semaphore_signal(ready, inc=1, device_id={"gy": gy + step}, device_id_type=MESH)

    start(X1, "gx", both(xs.at[0]), xr1)
    z_stage(vp, zs1)
    start(Z1, "agg", both(zs1), zr1)

    fetches[1].wait()
    reaction = r[...]
    c_ref[...] = damping / (6.0 + reaction)
    halved = reaction.reshape(4, 2, 16, 128)
    tp[0:64, :] = (halved[:, 0] + halved[:, 1]).reshape(64, 128)
    mean_r = dot(tp[pl.ds(0, 32, stride=2), :] + tp[pl.ds(1, 32, stride=2), :], halves)
    inverse = damping / ((6.0 + 4.0 * mean_r) * 0.25)
    down[...] = inverse
    stage_rows(down, y2s, 3, 1)
    for slot, (j, k) in faces:
        for c in range(3):
            y1s[slot, c] = plane(vp, c, j)
        y1s[slot, 3] = c_ref[pl.ds(j, 8, stride=16), :]
        y3s[slot, 3] = c_ref[pl.ds(k, 8, stride=16), :]
    send_y(Y1, y1s, y1r, sure)
    fetches[2].wait()
    fetches[3].wait()

    first = []
    for c in range(3):
        pairs = comp_of(vp, c).reshape(4, 2, 16, 128)
        first.append(((pairs[:, 0] + pairs[:, 1]) * root_half).reshape(64, 128))
    a1 = jnp.concatenate(first, axis=0)
    even = lax.rem(rows((192, 128)), 2) == 0
    a1 = jnp.where(even, a1 + pltpu.roll(a1, 191, 0), pltpu.roll(a1, 1, 0) - a1) * root_half
    out_z, in_z = rows((128, 128)), lane128
    same = lax.shift_right_logical(out_z, 1) == lax.shift_right_logical(in_z, 1)
    minus = jnp.logical_and(lax.rem(out_z, 2) == 1, lax.rem(in_z, 2) == 1)
    pass_z = jnp.where(same, jnp.where(minus, -root_half, root_half), 0.0).astype(F32)
    turned = jnp.concatenate([dot(pass_z, a1, ((1,), (1,))), jnp.zeros((128, 64), F32)], axis=1)
    for t in range(n_gx):
        sendt[t] = turned[t * per : (t + 1) * per, :]

    arrive(X1, "gx", both(xs.at[0]), xr1)
    arrive(Z1, "agg", both(zs1), zr1)
    z_low, z_high = zr1[0], zr1[1]
    for c in range(3):
        u = comp_of(vp, c)
        total = comp_of(f, c) + around(
            u, xr1[0, c], xr1[1, c], spread(z_low, c, 0), spread(z_high, c, 127)
        )
        u1[c * 128 : (c + 1) * 128, :] = keep * u + c_ref[...] * total
    x_stage(u1, 1)
    start(X2, "gx", both(xs.at[1]), xr2)
    z_stage(u1, zs2)
    start(Z2, "agg", both(zs2), zr2)
    for slot, (j, _) in faces:
        for c in range(3):
            y2s[slot, c] = plane(u1, c, j)
    send_y(Y2, y2s, y2r, sure)
    take_turn(1)

    arrive(X2, "gx", both(xs.at[1]), xr2)
    arrive(Z2, "agg", both(zs2), zr2)
    z_low, z_high = zr2[0], zr2[1]
    for c in range(3):
        u = comp_of(u1, c)
        total = comp_of(f, c) + around(
            u, xr2[0, c], xr2[1, c], spread(z_low, c, 0), spread(z_high, c, 127)
        )
        u2[c * 128 : (c + 1) * 128, :] = keep * u + c_ref[...] * total
    x_stage(u2, 2)
    even, odd = pl.ds(0, 8, stride=2), pl.ds(1, 8, stride=2)
    sums = [xs[2, side, c, even, :] + xs[2, side, c, odd, :] for side in (0, 1) for c in range(3)]
    sums = dot(jnp.concatenate(sums, axis=0), halves)
    for side in (0, 1):
        first, second, third = (sums[(side * 3 + c) * 8 : (side * 3 + c + 1) * 8] for c in range(3))
        xcs[side, 0] = jnp.where(lane8 < 64, first, pltpu.roll(second, 64, 1))
        xcs[side, 1] = third
    start(XC, "gx", both(xcs), xcr)
    z_stage(u2, zs3)
    start(Z3, "agg", both(zs3), zr3)
    for slot, (j, _) in faces:
        for c in range(3):
            y3s[slot, c] = plane(u2, c, j)
    send_y(Y3, y3s, y3r, sure)

    @pl.when(jnp.logical_or(later[0], later[1]))
    def _():
        pl.semaphore_wait(ready, 1)

    for message, src, dst in ((Y1, y1s, y1r), (Y2, y2s, y2r), (Y3, y3s, y3r)):
        send_y(message, src, dst, later)
        for side in (0, 1):
            ends.append((message, "gy", both(src), dst, side))
    take_turn(2)

    arrive(Z3, "agg", both(zs3), zr3)
    z3_low, z3_high = zr3[0], zr3[1]
    none = jnp.zeros((16, 128), F32)
    for c in range(3):
        u = comp_of(u2, c)
        res = (
            comp_of(f, c) - (6.0 + r[...]) * u
            + around(u, none, none, spread(z3_low, c, 0), spread(z3_high, c, 127))
        )
        halved = res.reshape(4, 2, 16, 128)
        tp[c * 64 : (c + 1) * 64, :] = (
            (halved[:, 0] + halved[:, 1]).reshape(64, 128)
        )
    bown[...] = dot(tp[pl.ds(0, 96, stride=2), :] + tp[pl.ds(1, 96, stride=2), :], halves)
    arrive(XC, "gx", both(xcs), xcr)
    for side, i in ((0, 0), (1, 3)):
        parts = (xcr[side, 0], pltpu.roll(xcr[side, 0], 64, 1), xcr[side, 1])
        for c in range(3):
            at = (c * 4 + i) * 8
            bown[at : at + 8, :] = bown[at : at + 8, :] + parts[c]
    stage_rows(bown, y4s, 0, 3)
    start(Y4, "gy", both(y4s), y4r)
    take_turn(3)


    arrive(Y1, "gy", both(y1s), y1r)
    take_turn(4)

    for side, (j, _) in mine:
        for c in range(3):
            k = side * 3 + c
            p1[k * 8 : k * 8 + 8, :] = c_ref[pl.ds(j, 8, stride=16), :] * y1r[side, c]
            p1[48 + k * 8 : 56 + k * 8, :] = y1r[side, 3] * plane(vp, c, j)
    xf2s[0, 0:12, :] = p1[pl.ds(7, 12, stride=8), :]
    xf2s[1, 0:12, :] = p1[pl.ds(0, 12, stride=8), :]
    start(XF2, "gx", both(xf2s), xf2r)
    tiles = [p1[k * 8 : k * 8 + 8, :] for k in range(12)]
    zf2s[0] = z_pack(tiles, 127, lane8)
    zf2s[1] = z_pack(tiles, 0, lane8)
    start(ZF2, "agg", both(zf2s), zf2r)

    start(X3, "gx", both(xs.at[2]), xr3)

    take_turn(5)

    def send_line(step, carry):
        target = lax.rem(gx + step, n_gx)
        pltpu.make_async_remote_copy(
            src_ref=sendt.at[target], dst_ref=recvt.at[gx],
            send_sem=assem, recv_sem=arsem, device_id={"gx": target}, device_id_type=MESH,
        ).start()
        return carry

    lax.fori_loop(1, n_gx, send_line, 0)

    arrive(XF2, "gx", both(xf2s), xf2r)
    arrive(ZF2, "agg", both(zf2s), zf2r)
    arrive(Y2, "gy", both(y2s), y2r)
    arrive(Y3, "gy", both(y3s), y3r)
    f2_low, f2_high = zf2r[0], zf2r[1]
    for side, (j, j1) in mine:
        c0, c1 = c_ref[pl.ds(j, 8, stride=16), :], c_ref[pl.ds(j1, 8, stride=16), :]
        ch0, ch1 = y1r[side, 3], y3r[side, 3]
        for c in range(3):
            k = side * 3 + c
            own, halo = p1[k * 8 : k * 8 + 8, :], p1[48 + k * 8 : 56 + k * 8, :]
            near = beside(own, k, xf2r, f2_low, f2_high) + y2r[side, c] + halo
            p2[k * 8 : k * 8 + 8, :] = keep * own + c0 * near
            p2[48 + k * 8 : 56 + k * 8, :] = c1 * own
            near = beside(halo, 6 + k, xf2r, f2_low, f2_high) + plane(u1, c, j) + own
            p2[96 + k * 8 : 104 + k * 8, :] = keep * halo + ch0 * near
            p2[144 + k * 8 : 152 + k * 8, :] = ch1 * halo
            po[k * 8 : k * 8 + 8, :] = damping * (keep * plane(vp, c, j) + near)
    xf3s[0] = p2[pl.ds(7, 24, stride=8), :]
    xf3s[1] = p2[pl.ds(0, 24, stride=8), :]
    start(XF3, "gx", both(xf3s), xf3r)
    tiles = [p2[k * 8 : k * 8 + 8, :] for k in range(24)]
    zf3s[0] = z_pack(tiles, 127, lane8)
    zf3s[1] = z_pack(tiles, 0, lane8)
    start(ZF3, "agg", both(zf3s), zf3r)

    unstage_rows(y2r, 3, dtile, 1)
    join(down, dtile, dpack, dzs, 1)
    start(DZ, "agg", both(dzs), dzr)
    start_corners(0)
    start(DX, "gx", (dpack, dpack), dxr)

    arrive(Y4, "gy", both(y4s), y4r)
    unstage_rows(y4r, 0, btile, 3)
    arrive(XF3, "gx", both(xf3s), xf3r)
    arrive(ZF3, "agg", both(zf3s), zf3r)
    f3_low, f3_high = zf3r[0], zf3r[1]
    for side, (j, j1) in mine:
        d0 = 6.0 + r[pl.ds(j, 8, stride=16), :]
        for c in range(3):
            k = side * 3 + c
            own0, own1, halo0, halo1 = (p2[n * 48 + k * 8 : n * 48 + k * 8 + 8, :] for n in range(4))
            whole0 = plane(u2, c, j) + own0
            beyond0 = y3r[side, c] + halo0
            near = beside(own0, k, xf3r, f3_low, f3_high) + beside(own1, 6 + k, xf3r, f3_low, f3_high)
            ps[k * 8 : k * 8 + 8, :] = (
                near + own1 + beyond0 + own0 - d0 * own0 - damping * p1[k * 8 : k * 8 + 8, :]
            )
            ps[48 + k * 8 : 56 + k * 8, :] = own1
            near = beside(halo0, 12 + k, xf3r, f3_low, f3_high) + beside(halo1, 18 + k, xf3r, f3_low, f3_high)
            ps[96 + k * 8 : 104 + k * 8, :] = (
                near + halo1 + whole0 + halo0 - po[k * 8 : k * 8 + 8, :] - damping * p1[48 + k * 8 : 56 + k * 8, :]
            )
            ps[144 + k * 8 : 152 + k * 8, :] = halo1
            put_plane(u2, c, j, whole0)
            put_plane(u2, c, j1, plane(u2, c, j1) + own1)
            ph[k * 8 : k * 8 + 8, :] = beyond0
    line = dot(ps[pl.ds(0, 96, stride=2), :] + ps[pl.ds(1, 96, stride=2), :], halves)
    for side in (0, 1):
        at0, at1 = ((0, 1), (7, 6))[side]
        to0, to1 = ((7, 6), (0, 1))[side]
        for c in range(3):
            k = (side * 3 + c) * 4
            for ref, row0, row1, base in ((bown, at0, at1, 0), (btile, to0, to1, 48)):
                for row, part in ((row0, k), (row1, 24 + k)):
                    at = pl.ds(c * 32 + row, 4, stride=8)
                    ref[at, :] = ref[at, :] + line[base + part : base + part + 4]
    join(bown, btile, bpack, bzs, 3)
    start(BZ, "agg", both(bzs), bzr)
    start_corners(1)
    start(BX, "gx", (bpack, bpack), bxr)


    many = n_gx - 1
    lines = pltpu.make_async_remote_copy(
        src_ref=sendt.at[pl.ds(0, many)], dst_ref=recvt.at[pl.ds(0, many)],
        send_sem=assem, recv_sem=arsem, device_id={"gx": lax.rem(gx + 1, n_gx)}, device_id_type=MESH,
    )
    lines.wait_recv()
    lines.wait_send()
    recvt[gx] = sendt[gx]
    for k in range(per):
        got = recvt[:, k, :]
        wide = dot(got[:, 0:192], mcat[...], ((0,), (0,)))
        for c in range(3):
            value = 0.0
            for m in range(4):
                at = (c * 4 + m) * 16
                value = value + wide[at : at + 16, m * 4 * n_gx : (m + 1) * 4 * n_gx]
            comp[c, :, k, :] = value

    arrive(DZ, "agg", both(dzs), dzr)
    arrive(DX, "gx", (dpack, dpack), dxr)
    arrive_corners(0)
    cdext[...] = assemble(dpack, dzr, dxr, dxz, 0, 1)
    arrive(BZ, "agg", both(bzs), bzr)
    arrive(BX, "gx", (bpack, bpack), bxr)
    arrive_corners(1)

    y16 = lax.rem(rows((192, 128)), 16)
    fine = lane128 // 2 == rows((128, 128))
    beyond = jnp.logical_or(
        jnp.logical_and(lane128 == 0, rows((128, 128)) == 127),
        jnp.logical_and(lane128 == 127, rows((128, 128)) == 64),
    )
    up = jnp.concatenate([jnp.where(fine, 1.0, 0.0), jnp.where(beyond, 1.0, 0.0)], axis=1).astype(F32)
    for c in range(3):
        rhs_c = assemble(bpack, bzr, bxr, bxz, c, 3)
        weight = cdext[...]
        e = weight * rhs_c
        for _ in range(COARSE_SWEEPS - 1):
            near = jnp.concatenate([none, e[:176]], axis=0) + jnp.concatenate([e[16:], none], axis=0)
            near = near + pltpu.roll(e, 1, 1) + pltpu.roll(e, 127, 1)
            near = near + jnp.where(y16 == 0, pltpu.roll(e, 192 - 15, 0), pltpu.roll(e, 1, 0))
            near = near + jnp.where(y16 == 15, pltpu.roll(e, 15, 0), pltpu.roll(e, 191, 0))
            e = keep * e + weight * (rhs_c + 0.25 * near)
        refined = dot(e[48:144], up)
        eu[c * 96 : (c + 1) * 96, :] = refined[:, 0:128]
        for ref, part in ((cf, refined[:, 0:128]), (cz, refined[:, 128:256])):
            main = part.reshape(6, 16, 128)[:, 0:8].reshape(48, 128)
            ref[pl.ds(c * 96, 48, stride=2), :] = main
            ref[pl.ds(c * 96 + 1, 48, stride=2), :] = main
        for side, row in ((0, 15), (1, 8)):
            line_ = eu[pl.ds(c * 96 + 16 + row, 4, stride=16), :]
            at = (side * 3 + c) * 8
            for step in (0, 1):
                spot = pl.ds(at + step, 4, stride=2)
                ph[spot, :] = ph[spot, :] + line_

    arrive(X3, "gx", both(xs.at[2]), xr3)

    def doubled(ref, c):
        value = ref[c * 96 + 16 : c * 96 + 80, :].reshape(4, 1, 16, 128)
        return jnp.broadcast_to(value, (4, 2, 16, 128)).reshape(128, 128)

    for c in range(3):
        w = comp_of(u2, c) + doubled(cf, c)
        outer = doubled(cz, c)
        total = comp_of(f, c) + around(
            w,
            xr3[0, c] + cf[c * 96 : c * 96 + 16, :],
            xr3[1, c] + cf[c * 96 + 80 : c * 96 + 96, :],
            spread(z3_low, c, 0) + outer,
            spread(z3_high, c, 127) + outer,
        )
        vel[c * 128 : (c + 1) * 128, :] = keep * w + c_ref[...] * total
    for side, (j, j1) in mine:
        c0, c1 = c_ref[pl.ds(j, 8, stride=16), :], c_ref[pl.ds(j1, 8, stride=16), :]
        for c in range(3):
            k = side * 3 + c
            more = edges(k, xf3r, f3_low, f3_high)
            more = more + ph[k * 8 : k * 8 + 8, :]
            put_plane(vel, c, j, plane(vel, c, j) + c0 * more)
            more = edges(6 + k, xf3r, f3_low, f3_high)
            put_plane(vel, c, j1, plane(vel, c, j1) + c1 * more)

    for message, axis, src, dst, side in ends:

        @pl.when(upper(axis) if side == 0 else lower(axis))
        def _(args=(message, axis, src, dst, side)):
            one_copy(*args).wait_send()

    for corner in corners:

        @pl.when(corner_there(*corner[2:]))
        def _(corner=corner):
            for kind in (0, 1):
                corner_copy(kind, *corner).wait_send()


def put_kernel(velocity, compressed, velocity_out, compressed_out, sem):
    copies = [
        pltpu.make_async_copy(velocity, velocity_out, sem.at[0]),
        pltpu.make_async_copy(compressed, compressed_out, sem.at[1]),
    ]
    for copy in copies:
        copy.start()
    for copy in copies:
        copy.wait()


def on_device(sizes, velocity_prev, forcing, reaction):
    n_agg, n_gx, n_gy = sizes
    per = 128 // n_gx

    def v(*shape):
        return pltpu.VMEM(shape, F32)

    scratch = [
        v(384, 128), v(384, 128), v(128, 128), v(n_gx, 16 * n_gx),
        v(128, 128), v(384, 128), v(384, 128), v(192, 128),
        v(n_gx, per, 256), v(n_gx, per, 256),
        v(3, 2, 3, 16, 128), v(2, 3, 16, 128), v(2, 3, 16, 128), v(2, 3, 16, 128),
        v(2, 2, 8, 128), v(2, 2, 8, 128),
    ]
    scratch += [v(2, 16, 128)] * 6
    scratch += [v(96, 128), v(192, 128), v(48, 128), v(192, 128)]
    scratch += [v(2, 16, 128)] * 2 + [v(2, 8, 128)] * 2 + [v(2, 24, 128)] * 2 + [v(2, 8, 128)] * 2
    scratch += [v(2, 4, 8, 128)] * 6 + [v(2, 3, 8, 128)] * 2
    for n in (1, 3):
        scratch += [v(n * 32, 128)] * 3 + [v(2, n * 32, 128), v(2, 8, 128), v(2, 8, 128), v(2, 2, 8, 128)]
    scratch += [v(192, 128), v(288, 128), v(288, 128), v(288, 128), v(48, 128)]
    dma = pltpu.SemaphoreType.DMA
    scratch += [dma((4,)), dma((COUNT, 2)), dma((COUNT, 2)), dma((2, 4)), dma((2, 4)), dma, dma]
    scratch += [pltpu.SemaphoreType.REGULAR] * 3
    vmem = pl.BlockSpec(memory_space=pltpu.VMEM)
    velocity, compressed = pl.pallas_call(
        functools.partial(kernel, sizes),
        out_shape=(
            jax.ShapeDtypeStruct((384, 128), F32),
            jax.ShapeDtypeStruct((3, 16, per, 4 * n_gx), F32),
        ),
        in_specs=[pl.BlockSpec(memory_space=pltpu.HBM)] * 4,
        out_specs=(vmem, vmem),
        scratch_shapes=scratch,
        compiler_params=pltpu.CompilerParams(
            collective_id=0, has_side_effects=True, vmem_limit_bytes=12 * 2**20
        ),
        name="vcycle",
    )(
        *(
            pltpu.with_memory_space_constraint(value, pltpu.HBM)
            for value in (
                velocity_prev.reshape(384, 128), forcing.reshape(384, 128), reaction.reshape(128, 128),
                jnp.asarray(haar_matrix(n_gx)),
            )
        )
    )
    velocity, compressed = pl.pallas_call(
        put_kernel,
        out_shape=tuple(jax.ShapeDtypeStruct(value.shape, F32) for value in (velocity, compressed)),
        in_specs=[vmem] * 2,
        out_specs=[pl.BlockSpec(memory_space=pltpu.HBM)] * 2,
        scratch_shapes=[dma((2,))],
        compiler_params=pltpu.CompilerParams(vmem_limit_bytes=12 * 2**20),
        name="put",
    )(velocity, compressed)
    return velocity.reshape(3, 8, 16, 128), compressed


def solution(mesh):
    placed = (P(None, "gx", "gy", "agg"), P(None, "gx", "gy", "agg"), P("gx", "gy", "agg"))
    sizes = tuple(mesh.shape[name] for name in ("agg", "gx", "gy"))
    return jax.shard_map(
        functools.partial(on_device, sizes),
        mesh=mesh,
        in_specs=placed,
        out_specs=(P(None, "gx", "gy", "agg"), P(None, "gy", ("agg", "gx"), None)),
        check_vma=False,
    )
```
